512 devices in a mesh: step: 16 (over y_lo, x), seq: 32 (over z, y_hi, core).
Axes of the slice: x: 4, y: 8 (y_hi: 2, y_lo: 4; y = y_hi * 4 + y_lo), z: 8, core: 2. Of those that a mesh axis runs over, the one named last changes fastest.
Arguments:
- latents: float32 [16, 1024, 64], P('step', 'seq'), may hold values from -6 to 6
- timesteps: int32 [17], replicated, may hold values from 0 to 1000, as said below
- embed_weight: bfloat16 [64, 4096], replicated, may hold values from -0.75 to 0.75
- mod_weight: float32 [256, 2, 4096], P('seq'), may hold values from -0.375 to 0.375
- qkv_weight: bfloat16 [4096, 32, 3, 128], P('step', 'seq'), may hold values from -0.09375 to 0.09375
- out_weight: bfloat16 [32, 128, 64], P('seq'), may hold values from -6 to 6
Outputs:
- updated: float32 [16, 1024, 64], P('step', 'seq')
- velocity: float32 [16, 1024, 64], P('step', 'seq')
The draws below stay inside these ranges and needn't reach their ends.
Inputs may be any that keep to these rules, and one draw needn't show every extreme that they name: `timesteps`: strictly decreasing along the table.
All inputs are finite; a program needn't handle non-finite values.
Results may differ from the reference program's by a relative error of at most 0.0049.
Values may be sent and summed in bfloat16 or wider, within the bound.
No kernel may reach another device: no remote copies, remote signals or barrier semaphores. Data moves between devices by JAX's collectives and lax.ppermute only.
A program may use at most 64 MiB of HBM per device.

```python
import math
import jax
import jax.numpy as jnp
from jax import lax

D = 4096
HD = 128
C = 64
FREQ = 256
HEADS = 32
STEPS = 16
TOKENS = 1024


def draw_timesteps(key, part):
    first_key, second_key = jax.random.split(jax.random.fold_in(key, 7))
    top_stamp = 1000 - jax.random.randint(first_key, (), 0, 40, dtype=jnp.int32)
    decrements = jax.random.randint(second_key, (STEPS,), 500 // STEPS, 900 // STEPS + 1, dtype=jnp.int32)
    cumulative = jnp.concatenate([jnp.zeros((1,), jnp.int32), jnp.cumsum(decrements).astype(jnp.int32)])
    return (top_stamp - cumulative).astype(jnp.int32)


def steps_of(own_key, shape, pieces, smallest, high):
    gain, own = 1.0, jax.random.fold_in(own_key, 6)
    for axis_at, parts in pieces:
        steps = jnp.exp(jax.random.uniform(jax.random.fold_in(own, axis_at), (parts,), jnp.float32, smallest / len(pieces), high / len(pieces)))
        gain = gain * jnp.repeat(steps, shape[axis_at] // parts).reshape([-1 if axis == axis_at else 1 for axis in range(len(shape))])
    return gain


def scatter_about(stream_key, dims, width, reach, shards=(), kind=jnp.bfloat16):
    level = steps_of(stream_key, dims, shards, -0.22, 0.18) if shards else 1.0
    entries = jax.random.normal(stream_key, dims, jnp.float32) * width * level
    return jnp.minimum(jnp.maximum(entries, -reach), reach).astype(kind)


def setup_inputs(seed: int = 0) -> dict:
    key_list = jax.random.split(jax.random.key(seed), 7)
    latents = scatter_about(key_list[0], (STEPS, TOKENS, C), 1.0, 6.0, ((0, 16), (1, 32)), jnp.float32)
    timesteps = draw_timesteps(jax.random.fold_in(key_list[6], 71), 0)
    embed_weight = scatter_about(key_list[2], (C, D), C ** -0.5, 0.75)
    mod_weight = scatter_about(key_list[3], (FREQ, 2, D), FREQ ** -0.5, 0.375, ((0, 32),), jnp.float32)
    qkv_weight = scatter_about(key_list[4], (D, HEADS, 3, HD), D ** -0.5, 0.09375, ((0, 16), (1, 32)))
    out_weight = scatter_about(key_list[5], (HEADS, HD, C), (1.2 * (TOKENS / (HEADS * HD)) ** 0.5), 6.0, ((0, 32),))
    return {"latents": latents, "timesteps": timesteps, "embed_weight": embed_weight, "mod_weight": mod_weight, "qkv_weight": qkv_weight, "out_weight": out_weight}


def condition_of(stamp):
    half_count = FREQ // 2
    frequencies = jnp.exp(-math.log(10000.0) * jnp.arange(half_count, dtype=jnp.float32) / half_count)
    angles = stamp * frequencies
    return jnp.concatenate([jnp.cos(angles), jnp.sin(angles)])

def modulate(latent_rows, embed_weight, shift_vec, scale_vec):
    embedded = jnp.dot(latent_rows, embed_weight, preferred_element_type=jnp.float32)
    center_mean = lax.optimization_barrier(jnp.mean(embedded, axis=-1, keepdims=True))
    centered = embedded - center_mean
    variance = lax.optimization_barrier(jnp.mean(centered * centered, axis=-1, keepdims=True))
    normed = centered * lax.rsqrt(variance + 1e-06)
    return (normed * (1.0 + shift_vec * 0.0 + scale_vec) + shift_vec).astype(jnp.bfloat16)

def qk_norm(head_rows):
    as_float = head_rows.astype(jnp.float32)
    return (as_float * lax.rsqrt(lax.optimization_barrier(jnp.mean(as_float * as_float, axis=-1, keepdims=True)) + 1e-06)).astype(jnp.bfloat16)

def attend_head(head_block):
    queries = qk_norm(head_block[:, 0])
    key_rows = qk_norm(head_block[:, 1])
    values = head_block[:, 2]
    seq_length = queries.shape[0]
    head_dim = queries.shape[1]
    block_rows = math.gcd(seq_length, 512)
    query_blocks = queries.reshape(seq_length // block_rows, block_rows, head_dim)

    def one_block(query_block):
        scores = jnp.dot(query_block, key_rows.T, preferred_element_type=jnp.float32) * (1.0 / math.sqrt(head_dim))
        weights = jnp.exp(scores)
        probabilities = (weights / lax.optimization_barrier(jnp.sum(weights, axis=-1, keepdims=True))).astype(jnp.bfloat16)
        return jnp.dot(probabilities, values, preferred_element_type=jnp.float32).astype(jnp.bfloat16)
    return lax.map(one_block, query_blocks).reshape(seq_length, head_dim)

def reference(latents, timesteps, embed_weight, mod_weight, qkv_weight, out_weight):
    stamps = timesteps.astype(jnp.float32)

    def one_step(inputs):
        latent_rows, stamp = inputs
        modulation = jnp.einsum('f,fcd->cd', condition_of(stamp), mod_weight, precision=lax.Precision.HIGHEST)
        modulated = modulate(latent_rows.astype(jnp.bfloat16), embed_weight, modulation[0], modulation[1])
        model_width = modulated.shape[1]
        seq_length = modulated.shape[0]
        projected = jnp.dot(modulated, qkv_weight.reshape(model_width, -1), preferred_element_type=jnp.float32)
        projected = projected.astype(jnp.bfloat16).reshape(seq_length, qkv_weight.shape[1], 3, qkv_weight.shape[3])
        attended = lax.map(attend_head, jnp.moveaxis(projected, 1, 0))
        return jnp.einsum('hsd,hdc->sc', attended.astype(jnp.float32), out_weight.astype(jnp.float32), precision=lax.Precision.HIGHEST)
    velocity = lax.map(one_step, (latents, stamps[:-1]))
    step_sizes = (stamps[1:] - stamps[:-1]) / 1000.0
    updated = latents[0][None] + jnp.cumsum(step_sizes[:, None, None] * velocity, axis=0)
    return (updated, velocity)
```

```python
import math

import jax
import jax.numpy as jnp
from jax import lax
from jax.experimental import pallas as pl
from jax.experimental.pallas import tpu as pltpu
from jax.sharding import Mesh
from jax.sharding import PartitionSpec as P

STEP = ("y_lo", "x")
SEQ = ("z", "y_hi", "core")
BF = jnp.bfloat16
F32 = jnp.float32
LN = 128
SMEM = pltpu.SMEM


def dot(a, b):
    return jnp.dot(a, b, preferred_element_type=F32)


def dot_t(a, b):
    return lax.dot_general(a, b, (((1,), (1,)), ((), ())), preferred_element_type=F32)


def halves(x):
    hi = x.astype(BF)
    return hi, (x - hi.astype(F32)).astype(BF)


def low_lanes(shape):
    return lax.broadcasted_iota(jnp.int32, shape, len(shape) - 1) < LN // 2


def pack_rows(rows):
    return jnp.concatenate([rows[:16], rows[16:]], axis=1)


def pack_kernel(at_ref, lat_ref, mw_ref, out_ref):
    lat = pack_rows(lat_ref[0]).astype(BF)
    by_kind = [mw_ref[:, 0, :], mw_ref[:, 1, :]]
    blocks = [lat]
    lows = []
    for part in range(2):
        cols = slice(part * LN, (part + 1) * LN)
        hi, lo = halves(jnp.concatenate([by_kind[0][:, cols], by_kind[1][:, cols]], axis=0))
        blocks.append(hi)
        lows.append(lo)
    payload = jnp.concatenate(blocks + lows, axis=0)
    for peer in range(out_ref.shape[0]):
        out_ref[peer] = payload


def pack(at, latents, mod_weight, peers):
    width = mod_weight.shape[2] // 16
    return pl.pallas_call(
        pack_kernel,
        grid_spec=pltpu.PrefetchScalarGridSpec(
            num_scalar_prefetch=1,
            grid=(1,),
            in_specs=[
                pl.BlockSpec(latents.shape, lambda i, at: (0, 0, 0)),
                pl.BlockSpec((8, 2, width), lambda i, at: (0, 0, at[0])),
            ],
            out_specs=pl.BlockSpec((peers, 80, LN), lambda i, at: (0, 0, 0)),
        ),
        out_shape=jax.ShapeDtypeStruct((peers, 80, LN), BF),
        name="pack",
    )(at, latents, mod_weight)


def weights_kernel(at_ref, embed_ref, part_ref, w_ref, out_ref, centered_ref, gram_ref, wv_ref):
    embed = embed_ref[...].astype(F32)
    mean = jnp.mean(embed, axis=1, keepdims=True)
    centered_ref[...] = part_ref[...].astype(F32) - mean
    hi, lo = halves(embed - mean)
    hi2 = jnp.concatenate([hi, hi], axis=0)
    lo2 = jnp.concatenate([lo, lo], axis=0)
    gram = (dot_t(hi2, hi2) + dot_t(hi2, lo2) + dot_t(lo2, hi2)) * (1.0 / embed.shape[1])
    row = lax.broadcasted_iota(jnp.int32, gram.shape, 0) < LN // 2
    gram = jnp.where(row == low_lanes(gram.shape), gram, 0.0)
    gram_ref[0], gram_ref[1] = halves(gram)
    out = out_ref[0]
    wv_ref[0], wv_ref[1] = halves(dot(w_ref[...], jnp.concatenate([out, out], axis=1)))


def weights(at, embed_weight, wv, out_weight):
    width = wv.shape[0]
    channels = embed_weight.shape[0]
    return pl.pallas_call(
        weights_kernel,
        grid_spec=pltpu.PrefetchScalarGridSpec(
            num_scalar_prefetch=1,
            grid=(1,),
            in_specs=[
                pl.BlockSpec(embed_weight.shape, lambda i, at: (0, 0)),
                pl.BlockSpec((channels, width), lambda i, at: (0, at[0])),
                pl.BlockSpec(wv.shape, lambda i, at: (0, 0)),
                pl.BlockSpec(out_weight.shape, lambda i, at: (0, 0, 0)),
            ],
            out_specs=[
                pl.BlockSpec((channels, width), lambda i, at: (0, 0)),
                pl.BlockSpec((2, LN, LN), lambda i, at: (0, 0, 0)),
                pl.BlockSpec((2, width, LN), lambda i, at: (0, 0, 0)),
            ],
        ),
        out_shape=[
            jax.ShapeDtypeStruct((channels, width), F32),
            jax.ShapeDtypeStruct((2, LN, LN), BF),
            jax.ShapeDtypeStruct((2, width, LN), BF),
        ],
        name="weights",
    )(at, embed_weight, embed_weight, wv, out_weight)


def partial_kernel(mod_ref, cond_ref, centered_ref, w_ref, wv_ref, out_ref):
    cond = cond_ref[...]
    cond_hi, cond_lo = halves(cond)
    cond2 = jnp.concatenate([cond_hi, cond_lo], axis=0)
    parts = []
    for part in range(2):
        hi = mod_ref[:, :, 16 + part * 16 : 32 + part * 16, :].reshape(512, LN)
        lo = mod_ref[:, :, 48 + part * 16 : 64 + part * 16, :].reshape(512, LN)
        both = dot(cond2, hi)
        parts.append(both[:32] + both[32:] + dot(cond_hi, lo))
    modulation = jnp.concatenate(parts, axis=1)
    shift, scale = modulation[:16], modulation[16:] + 1.0
    centered = centered_ref[...]
    rows = jnp.concatenate(
        [(centered * scale[k : k + 1]).astype(BF) for k in range(16)], axis=0
    )
    shift2 = jnp.concatenate(halves(shift), axis=0)
    wq, wk, wv_hi, wv_lo = w_ref[0], w_ref[1], wv_ref[0], wv_ref[1]
    mq = dot(rows, wq)
    mk = dot(rows, wk)
    mv = dot(rows, wv_hi) + dot(rows, wv_lo)
    biases = []
    for w in (wq, wk, wv_hi):
        b = dot(shift2, w)
        biases.append(b[:16] + b[16:])
    biases[2] = biases[2] + dot(shift2[:16], wv_lo)
    line = lax.broadcasted_iota(jnp.int32, (16, LN), 0)
    low = low_lanes((32, LN))
    for k in range(16):
        at = slice(k * 64, k * 64 + 64)
        out_ref[k, 0:64] = mq[at].astype(BF)
        out_ref[k, 64:128] = mk[at].astype(BF)
        v = mv[at]
        out_ref[k, 128:160] = jnp.where(low, v[:32], v[32:]).astype(BF)
        tile = jnp.where(line == 0, biases[0][k : k + 1], 0.0)
        tile = jnp.where(line == 1, biases[1][k : k + 1], tile)
        tile = jnp.where(line == 2, biases[2][k : k + 1], tile)
        out_ref[k, 160:176] = tile.astype(BF)


def attend_kernel(parts_ref, lat_ref, gram_ref, out_ref):
    total = jnp.sum(parts_ref[...].astype(F32), axis=0)
    mq, mk, mv = total[0:64], total[64:128], total[128:160]
    low32 = low_lanes((32, LN))
    turned = pltpu.roll(mv, LN // 2, 1)
    mv = jnp.concatenate(
        [jnp.where(low32, mv, turned), jnp.where(low32, turned, mv)], axis=0
    )
    bias_q, bias_k, bias_v = total[160:161], total[161:162], total[162:163]
    packed = lat_ref[...].reshape(512, LN)
    as_float = packed.astype(F32)
    square = (dot(packed, gram_ref[0]) + dot(packed, gram_ref[1])) * as_float
    low = low_lanes((512, LN))
    gain_low = lax.rsqrt(jnp.sum(jnp.where(low, square, 0.0), axis=1, keepdims=True) + 1e-06)
    gain_high = lax.rsqrt(jnp.sum(jnp.where(low, 0.0, square), axis=1, keepdims=True) + 1e-06)
    twice = jnp.concatenate([packed, packed], axis=1)
    none = jnp.zeros((64, LN), BF)

    def project(m, bias):
        hi, lo = halves(m)
        first = dot(twice, jnp.concatenate([hi, none, lo, none], axis=0))
        second = dot(twice, jnp.concatenate([none, hi, none, lo], axis=0))
        return gain_low * first + bias, gain_high * second + bias

    def unit(u, factor):
        mean = jnp.mean(u * u, axis=1, keepdims=True)
        return (u * (lax.rsqrt(mean + 1e-06) * factor)).astype(BF)

    q_low, q_high = (unit(u, math.log2(math.e) / math.sqrt(128)) for u in project(mq, bias_q))
    keys = jnp.concatenate([unit(u, 1.0) for u in project(mk, bias_k)], axis=0)
    values = jnp.concatenate(project(mv, bias_v), axis=0)
    all_low = low_lanes((1024, LN))
    values_low = jnp.where(all_low, values, 1.0).astype(BF)
    values_high = jnp.where(all_low, 1.0, values).astype(BF)

    def attend(q, v):
        return dot(jnp.exp2(dot_t(q, keys)).astype(BF), v)

    side = low_lanes((256, LN))
    for core in range(2):
        at = slice(core * 256, core * 256 + 256)
        first = attend(q_low[at], values_low)
        second = attend(q_high[at], values_high)
        over = jnp.where(side, first, second)
        under = pltpu.roll(jnp.where(side, second, first), LN // 2, 1)
        shares = (over / under).astype(BF)
        for z in range(8):
            out_ref[z * 2 + core] = shares[z * 32 : z * 32 + 32]


def step_of(stamps_ref, step):
    width = jnp.full((16, LN), stamps_ref[step + 1] - stamps_ref[step], jnp.int32)
    return width.astype(F32) / 1000.0


def increments_kernel(at_ref, stamps_ref, shares_ref, lat_ref, out_ref, own_ref):
    step, side = at_ref[0], at_ref[1]
    velocity = jnp.sum(shares_ref[...].astype(F32), axis=0)
    size = step_of(stamps_ref, step)
    start = jnp.where(step == 0, pack_rows(lat_ref[0]), 0.0)
    for part in range(2):
        mine = velocity[part * 16 : part * 16 + 16]
        grown = size * mine
        grown = jnp.where(side == part, grown + start, grown).astype(BF)
        for peer in range(16):
            out_ref[peer * 2 + part] = grown
    own_ref[...] = jnp.where(side == 0, velocity[:16], velocity[16:])


def finish_kernel(at_ref, stamps_ref, terms_ref, own_ref, lat_ref, updated_ref, velocity_ref):
    step, side = at_ref[0], at_ref[1]
    own = own_ref[...]
    size = step_of(stamps_ref, step)
    other = terms_ref[step * 2 + 1 - side].astype(F32)
    start = jnp.where(step == 0, pack_rows(lat_ref[0]), 0.0)
    velocity = own + other / size
    updated = size * own + start + other
    for j in range(15):
        term = terms_ref[2 * j].astype(F32) + terms_ref[2 * j + 1].astype(F32)
        updated = updated + jnp.where(j < step, term, 0.0)
    for ref, value in ((updated_ref, updated), (velocity_ref, velocity)):
        ref[0, 0:16] = value[:, : LN // 2]
        ref[0, 16:32] = pltpu.roll(value, LN // 2, 1)[:, : LN // 2]


def condition_table(timesteps):
    shape = (32, 512)
    col = lax.broadcasted_iota(jnp.int32, shape, 1)
    row = lax.broadcasted_iota(jnp.int32, shape, 0)
    source = col // 16
    feature = ((source % 16) * 2 + source // 16) * 8 + col % 8
    half_count = 128
    place = (feature % half_count).astype(F32)
    frequencies = jnp.exp(-math.log(10000.0) * place / half_count)
    stamps = jnp.tile(timesteps[:16].astype(F32), 2)
    angles = stamps[:, None] * frequencies
    value = jnp.where(feature < half_count, jnp.cos(angles), jnp.sin(angles))
    return jnp.where(row // 16 == (col // 8) % 2, value, 0.0)


def call(kernel, out_shape, name, scalars, *args):
    smem = pl.BlockSpec(memory_space=SMEM)
    vmem = pl.BlockSpec(memory_space=pltpu.VMEM)
    return pl.pallas_call(
        kernel,
        in_specs=[smem] * len(scalars) + [vmem] * len(args),
        out_shape=out_shape,
        name=name,
    )(*scalars, *args)


def on_device(latents, timesteps, embed_weight, mod_weight, qkv_weight, out_weight):
    at = jnp.stack([lax.axis_index(STEP), lax.axis_index("y_hi")]).astype(jnp.int32)
    payload = pack(at, latents, mod_weight, 16)
    payload = lax.all_to_all(payload, ("z", "y_hi"), 0, 0, tiled=True)
    everything = lax.all_gather(payload, "core")
    table = condition_table(timesteps)
    w = jnp.moveaxis(qkv_weight[:, 0], 1, 0)
    centered, gram, wv = weights(at, embed_weight, w[2], out_weight)
    parts = call(
        partial_kernel,
        jax.ShapeDtypeStruct((16, 176, LN), BF),
        "partial",
        (),
        everything,
        table,
        centered,
        w,
        wv,
    )
    parts = lax.all_to_all(parts, STEP, 0, 0, tiled=True)
    shares = pl.pallas_call(
        attend_kernel,
        grid=(1,),
        in_specs=[
            pl.BlockSpec((16, 176, LN), lambda i: (0, 0, 0)),
            pl.BlockSpec((2, 16, 16, LN), lambda i: (0, 0, 0, 0)),
            pl.BlockSpec((2, LN, LN), lambda i: (0, 0, 0)),
        ],
        out_specs=pl.BlockSpec((16, 32, LN), lambda i: (0, 0, 0)),
        out_shape=jax.ShapeDtypeStruct((16, 32, LN), BF),
        name="attend",
    )(parts, everything, gram)
    shares = lax.all_to_all(shares, ("z", "core"), 0, 0, tiled=True)
    terms, own = call(
        increments_kernel,
        [jax.ShapeDtypeStruct((32, 16, LN), BF), jax.ShapeDtypeStruct((16, LN), F32)],
        "increments",
        (at, timesteps),
        shares,
        latents,
    )
    terms = lax.all_to_all(terms, ("y_lo", "x", "y_hi"), 0, 0, tiled=True)
    out = jax.ShapeDtypeStruct(latents.shape, F32)
    updated, velocity = call(
        finish_kernel, [out, out], "finish", (at, timesteps), terms, own, latents
    )
    return updated, velocity


def solution(mesh):
    split = Mesh(mesh.devices.reshape(4, 4, 8, 2, 2), STEP + SEQ)
    return jax.shard_map(
        on_device,
        mesh=split,
        in_specs=(
            P(STEP, SEQ, None),
            P(),
            P(),
            P(SEQ, None, None),
            P(STEP, SEQ, None, None),
            P(SEQ, None, None),
        ),
        out_specs=(P(STEP, SEQ, None), P(STEP, SEQ, None)),
        check_vma=False,
    )
```

```python
import math

import jax
import jax.numpy as jnp
from jax import lax
from jax.experimental import pallas as pl
from jax.experimental.pallas import tpu as pltpu
from jax.sharding import Mesh
from jax.sharding import PartitionSpec as P


STEP = ("y_lo", "x")
SEQ = ("z", "y_hi", "core")
BF = jnp.bfloat16
F32 = jnp.float32
LN = 128


def dot(a, b):
    return jnp.dot(a, b, preferred_element_type=F32)


def dot_t(a, b):
    return lax.dot_general(a, b, (((1,), (1,)), ((), ())), preferred_element_type=F32)


def halves(x):
    hi = x.astype(BF)
    return hi, (x - hi.astype(F32)).astype(BF)


def low_lanes(shape):
    return lax.broadcasted_iota(jnp.int32, shape, len(shape) - 1) < LN // 2


def pack_rows(rows):
    return jnp.concatenate([rows[:16], rows[16:]], axis=1)


def place(*axes):
    index = 0
    for axis in axes:
        index = index * lax.axis_size(axis) + lax.axis_index(axis)
    return index


def own_columns():
    return pl.ds(pl.multiple_of(place("y_lo") * 1024, 1024), 1024)


def conditions(stamps_ref):
    shape = (8, 16)
    row = lax.broadcasted_iota(jnp.int32, shape, 0)
    col = lax.broadcasted_iota(jnp.int32, shape, 1)
    stamp = jnp.zeros(shape, jnp.int32)
    for k in range(4):
        stamp = jnp.where(row % 4 == k, stamps_ref[k * 4 + place("x")], stamp)
    feature = place(*SEQ) * 8 + col % 8
    half_count = 128
    frequencies = jnp.exp(-math.log(10000.0) * (feature % half_count).astype(F32) / half_count)
    angles = stamp.astype(F32) * frequencies
    value = jnp.where(feature < half_count, jnp.cos(angles), jnp.sin(angles))
    return jnp.where(row // 4 == col // 8, value, 0.0)


def pack_kernel(stamps_ref, lat_ref, mw_ref, out_ref):
    lat = pack_rows(lat_ref[0]).astype(BF)
    own = own_columns()
    cond_hi, cond_lo = halves(conditions(stamps_ref))
    hi, lo = halves(jnp.concatenate([mw_ref[:, 0, own], mw_ref[:, 1, own]], axis=0))
    share = dot(cond_hi, hi) + dot(cond_lo, hi) + dot(cond_hi, lo)
    blocks = [share[:, part * LN : (part + 1) * LN] for part in range(8)]
    payload = jnp.concatenate([lat, jnp.concatenate(blocks, axis=0).astype(BF)], axis=0)
    for peer in range(out_ref.shape[0]):
        out_ref[peer] = payload


def weights_kernel(embed_ref, centered_ref, gram_ref):
    embed = embed_ref[...].astype(F32)
    mean = jnp.mean(embed, axis=1, keepdims=True)
    centered_ref[...] = embed_ref[:, own_columns()].astype(F32) - mean
    hi, lo = halves(embed - mean)
    hi2 = jnp.concatenate([hi, hi], axis=0)
    lo2 = jnp.concatenate([lo, lo], axis=0)
    gram = (dot_t(hi2, hi2) + dot_t(hi2, lo2) + dot_t(lo2, hi2)) * (1.0 / embed.shape[1])
    row = lax.broadcasted_iota(jnp.int32, gram.shape, 0) < LN // 2
    gram = jnp.where(row == low_lanes(gram.shape), gram, 0.0)
    gram_ref[0], gram_ref[1] = halves(gram)


def partial_kernel(mod_ref, centered_ref, out_weight_ref, *refs):
    w_refs, out_ref, modulation_ref = refs[:4], refs[4], refs[5]
    total = jnp.sum(mod_ref[:, 16:80, :].astype(F32), axis=0)
    for part in range(8):
        modulation_ref[:, part * LN : (part + 1) * LN] = total[part * 8 : part * 8 + 8]
    out = out_weight_ref[0]
    out = jnp.concatenate([out, out], axis=0)
    mq = mk = mv = 0.0
    biases = [0.0, 0.0, 0.0]
    for far, w_ref in enumerate(w_refs):
        origin = lax.rem(place("x") + 4 - far, 4)
        own = pl.ds(pl.multiple_of(origin * 256, 256), 256)
        modulation = modulation_ref[:, own]
        shift, scale = modulation[:4], modulation[4:] + 1.0
        centered = centered_ref[:, own]
        rows = jnp.concatenate(
            [(centered * scale[k : k + 1]).astype(BF) for k in range(4)], axis=0
        )
        shift2 = jnp.concatenate(halves(shift), axis=0)
        wq, wk, wv = w_ref[0:256], w_ref[256:512], w_ref[512:768]
        wv_hi, wv_lo = halves(dot_t(wv, out))
        mq = mq + dot(rows, wq)
        mk = mk + dot(rows, wk)
        mv = mv + dot(rows, wv_hi) + dot(rows, wv_lo)
        for j, w in enumerate((wq, wk, wv_hi)):
            b = dot(shift2, w)
            biases[j] = biases[j] + b[:4] + b[4:]
        biases[2] = biases[2] + dot(shift2, wv_lo)[:4]
    line = lax.broadcasted_iota(jnp.int32, (16, LN), 0)
    low = low_lanes((32, LN))
    for k in range(4):
        at = slice(k * 64, k * 64 + 64)
        out_ref[k, 0:64] = mq[at].astype(BF)
        out_ref[k, 64:128] = mk[at].astype(BF)
        v = mv[at]
        out_ref[k, 128:160] = jnp.where(low, v[:32], v[32:]).astype(BF)
        tile = jnp.where(line == 0, biases[0][k : k + 1], 0.0)
        tile = jnp.where(line == 1, biases[1][k : k + 1], tile)
        tile = jnp.where(line == 2, biases[2][k : k + 1], tile)
        out_ref[k, 160:176] = tile.astype(BF)


def attend_kernel(parts_ref, lat_ref, gram_ref, out_ref):
    total = jnp.sum(parts_ref[...].astype(F32), axis=0)
    mq, mk, mv = total[0:64], total[64:128], total[128:160]
    low32 = low_lanes((32, LN))
    turned = pltpu.roll(mv, LN // 2, 1)
    mv = jnp.concatenate(
        [jnp.where(low32, mv, turned), jnp.where(low32, turned, mv)], axis=0
    )
    bias_q, bias_k, bias_v = total[160:161], total[161:162], total[162:163]
    packed = lat_ref[:, 0:16, :].reshape(512, LN)
    as_float = packed.astype(F32)
    square = (dot(packed, gram_ref[0]) + dot(packed, gram_ref[1])) * as_float
    low = low_lanes((512, LN))
    gain_low = lax.rsqrt(jnp.sum(jnp.where(low, square, 0.0), axis=1, keepdims=True) + 1e-06)
    gain_high = lax.rsqrt(jnp.sum(jnp.where(low, 0.0, square), axis=1, keepdims=True) + 1e-06)
    twice = jnp.concatenate([packed, packed], axis=1)
    none = jnp.zeros((64, LN), BF)

    def project(m, bias):
        hi, lo = halves(m)
        first = dot(twice, jnp.concatenate([hi, none, lo, none], axis=0))
        second = dot(twice, jnp.concatenate([none, hi, none, lo], axis=0))
        return gain_low * first + bias, gain_high * second + bias

    def unit(u, factor):
        mean = jnp.mean(u * u, axis=1, keepdims=True)
        return (u * (lax.rsqrt(mean + 1e-06) * factor)).astype(BF)

    q_low, q_high = (unit(u, math.log2(math.e) / math.sqrt(128)) for u in project(mq, bias_q))
    keys = jnp.concatenate([unit(u, 1.0) for u in project(mk, bias_k)], axis=0)
    values = jnp.concatenate(project(mv, bias_v), axis=0)
    all_low = low_lanes((1024, LN))
    values_low = jnp.where(all_low, values, 1.0).astype(BF)
    values_high = jnp.where(all_low, 1.0, values).astype(BF)

    def attend(q, v):
        return dot(jnp.exp2(dot_t(q, keys)).astype(BF), v)

    side = low_lanes((256, LN))
    for core in range(2):
        at = slice(core * 256, core * 256 + 256)
        first = attend(q_low[at], values_low)
        second = attend(q_high[at], values_high)
        over = jnp.where(side, first, second)
        under = pltpu.roll(jnp.where(side, second, first), LN // 2, 1)
        shares = (over / under).astype(BF)
        for z in range(8):
            out_ref[z * 2 + core] = shares[z * 32 : z * 32 + 32]


def step_of(stamps_ref, step):
    width = jnp.full((16, LN), stamps_ref[step + 1] - stamps_ref[step], jnp.int32)
    return width.astype(F32) / 1000.0


def increments_kernel(stamps_ref, shares_ref, lat_ref, out_ref, own_ref):
    step, side = place(*STEP), place("y_hi")
    velocity = jnp.sum(shares_ref[...].astype(F32), axis=0)
    size = step_of(stamps_ref, step)
    start = jnp.where(step == 0, pack_rows(lat_ref[0]), 0.0)
    for part in range(2):
        mine = velocity[part * 16 : part * 16 + 16]
        grown = size * mine
        grown = jnp.where(side == part, grown + start, grown).astype(BF)
        for peer in range(16):
            out_ref[peer * 2 + part] = grown
    own_ref[...] = jnp.where(side == 0, velocity[:16], velocity[16:])


def finish_kernel(stamps_ref, terms_ref, own_ref, lat_ref, updated_ref, velocity_ref):
    step, side = place(*STEP), place("y_hi")
    own = own_ref[...]
    size = step_of(stamps_ref, step)
    other = terms_ref[step * 2 + 1 - side].astype(F32)
    start = jnp.where(step == 0, pack_rows(lat_ref[0]), 0.0)
    velocity = own + other / size
    updated = size * own + start + other
    for j in range(15):
        term = terms_ref[2 * j].astype(F32) + terms_ref[2 * j + 1].astype(F32)
        updated = updated + jnp.where(j < step, term, 0.0)
    for ref, value in ((updated_ref, updated), (velocity_ref, velocity)):
        ref[0, 0:16] = value[:, : LN // 2]
        ref[0, 16:32] = pltpu.roll(value, LN // 2, 1)[:, : LN // 2]


def near(x):
    return pltpu.with_memory_space_constraint(x, pltpu.VMEM)


def call(kernel, outs, *args, scalars=(), scratch=()):
    smem = pl.BlockSpec(memory_space=pltpu.SMEM)
    vmem = pl.BlockSpec(memory_space=pltpu.VMEM)
    return pl.pallas_call(
        kernel,
        in_specs=[smem] * len(scalars) + [vmem] * len(args),
        out_specs=[vmem] * len(outs),
        out_shape=outs,
        scratch_shapes=scratch,
    )(*scalars, *args)


def stages(latents, timesteps, embed_weight, mod_weight, qkv_weight, out_weight):
    vmem = pltpu.VMEM
    (payload,) = call(
        pack_kernel, [vmem((16, 80, LN), BF)], latents, mod_weight, scalars=(timesteps,)
    )
    payload = lax.all_to_all(payload, ("z", "y_hi"), 0, 0, tiled=True)
    gathered = near(lax.all_gather(payload, "core", tiled=True))
    w = jnp.moveaxis(qkv_weight[:, 0], 1, 0).reshape(768, LN)
    ws = [w] + [lax.ppermute(w, "x", [(i, (i + far) % 4) for i in range(4)]) for far in (1, 2, 3)]
    centered, gram = call(
        weights_kernel, [vmem((64, 1024), F32), vmem((2, LN, LN), BF)], embed_weight
    )
    (parts,) = call(
        partial_kernel,
        [vmem((4, 176, LN), BF)],
        gathered,
        near(centered),
        near(jnp.swapaxes(out_weight, 1, 2)),
        *[near(w) for w in ws],
        scratch=[vmem((8, 1024), F32)],
    )
    parts = near(lax.all_to_all(parts, "y_lo", 0, 0, tiled=True))
    (shares,) = call(attend_kernel, [vmem((16, 32, LN), BF)], parts, gathered, near(gram))
    shares = near(lax.all_to_all(shares, ("z", "core"), 0, 0, tiled=True))
    terms, own = call(
        increments_kernel,
        [vmem((32, 16, LN), BF), vmem((16, LN), F32)],
        shares,
        latents,
        scalars=(timesteps,),
    )
    terms = near(lax.all_to_all(terms, ("y_lo", "x", "y_hi"), 0, 0, tiled=True))
    out = jax.ShapeDtypeStruct(latents.shape, F32)
    return tuple(
        call(finish_kernel, [out, out], terms, near(own), latents, scalars=(timesteps,))
    )


def solution(mesh):
    split = Mesh(mesh.devices.reshape(4, 4, 8, 2, 2), STEP + SEQ)
    return jax.shard_map(
        stages,
        mesh=split,
        in_specs=(
            P(STEP, SEQ, None),
            P(),
            P(),
            P(SEQ, None, None),
            P(STEP, SEQ, None, None),
            P(SEQ, None, None),
        ),
        out_specs=(P(STEP, SEQ, None), P(STEP, SEQ, None)),
        check_vma=False,
    )
```

```python
import math

import jax
import jax.numpy as jnp
from jax import lax
from jax.experimental import pallas as pl
from jax.experimental.pallas import tpu as pltpu
from jax.sharding import Mesh
from jax.sharding import PartitionSpec as P


STEP = ("y_lo", "x")
SEQ = ("z", "y_hi", "core")
BF = jnp.bfloat16
F32 = jnp.float32
LN = 128


def dot(a, b):
    return jnp.dot(a, b, preferred_element_type=F32)


def dot_t(a, b):
    return lax.dot_general(a, b, (((1,), (1,)), ((), ())), preferred_element_type=F32)


def halves(x):
    hi = x.astype(BF)
    return hi, (x - hi.astype(F32)).astype(BF)


def low_lanes(shape):
    return lax.broadcasted_iota(jnp.int32, shape, len(shape) - 1) < LN // 2


def pack_rows(rows):
    return jnp.concatenate([rows[:16], rows[16:]], axis=1)


def place(*axes):
    index = 0
    for axis in axes:
        index = index * lax.axis_size(axis) + lax.axis_index(axis)
    return index


def own_columns():
    return pl.ds(pl.multiple_of(place("y_lo") * 1024, 1024), 1024)


def conditions(stamps_ref):
    shape = (8, 16)
    row = lax.broadcasted_iota(jnp.int32, shape, 0)
    col = lax.broadcasted_iota(jnp.int32, shape, 1)
    stamp = jnp.zeros(shape, jnp.int32)
    for k in range(4):
        stamp = jnp.where(row % 4 == k, stamps_ref[k * 4 + place("x")], stamp)
    feature = place(*SEQ) * 8 + col % 8
    half_count = 128
    frequencies = jnp.exp(-math.log(10000.0) * (feature % half_count).astype(F32) / half_count)
    angles = stamp.astype(F32) * frequencies
    value = jnp.where(feature < half_count, jnp.cos(angles), jnp.sin(angles))
    return jnp.where(row // 4 == col // 8, value, 0.0)


def twin(lines):
    low = low_lanes(lines.shape)
    turned = pltpu.roll(lines, LN // 2, 1)
    return jnp.concatenate([jnp.where(low, lines, turned), jnp.where(low, turned, lines)], axis=0)


def pack_kernel(stamps_ref, lat_ref, mw_ref, w_ref, out_weight_ref, out_ref, folded_ref):
    out = out_weight_ref[0]
    wv = dot_t(w_ref[2], jnp.concatenate([out, out], axis=0))
    folded_ref[0:512] = w_ref[0:2].reshape(512, LN)
    folded_ref[512:640] = jnp.where(low_lanes((LN, LN)), wv[:LN], wv[LN:]).astype(BF)
    lat = pack_rows(lat_ref[0]).astype(BF)
    own = own_columns()
    cond_hi, cond_lo = halves(conditions(stamps_ref))
    hi, lo = halves(jnp.concatenate([mw_ref[:, 0, own], mw_ref[:, 1, own]], axis=0))
    share = dot(cond_hi, hi) + dot(cond_lo, hi) + dot(cond_hi, lo)
    blocks = [share[:, part * LN : (part + 1) * LN] for part in range(8)]
    payload = jnp.concatenate([lat, jnp.concatenate(blocks, axis=0).astype(BF)], axis=0)
    for peer in range(out_ref.shape[0]):
        out_ref[peer] = payload


def weights_kernel(embed_ref, centered_ref, gram_ref):
    embed = embed_ref[...].astype(F32)
    mean = jnp.mean(embed, axis=1, keepdims=True)
    centered_ref[...] = embed_ref[:, own_columns()].astype(F32) - mean
    hi, lo = halves(embed - mean)
    products = dot_t(jnp.concatenate([hi, lo], axis=0), hi)
    cross = products[64:]
    gram = (products[:64] + cross + cross.T) * (1.0 / embed.shape[1])
    none = jnp.zeros_like(gram)
    gram = jnp.concatenate(
        [jnp.concatenate([gram, none], axis=1), jnp.concatenate([none, gram], axis=1)], axis=0
    )
    gram_ref[0], gram_ref[1] = halves(gram)


def partial_kernel(mod_ref, centered_ref, *refs):
    w_refs, out_ref, modulation_ref = refs[:4], refs[4], refs[5]
    total = jnp.sum(mod_ref[:, 16:80, :].astype(F32), axis=0)
    for part in range(8):
        modulation_ref[:, part * LN : (part + 1) * LN] = total[part * 8 : part * 8 + 8]
    mq = mk = mv = 0.0
    biases = [0.0, 0.0, 0.0]
    for far, w_ref in enumerate(w_refs):
        origin = lax.rem(place("x") + 4 - far, 4)
        own = pl.ds(pl.multiple_of(origin * 256, 256), 256)
        modulation = modulation_ref[:, own]
        shift, scale = modulation[:4], modulation[4:] + 1.0
        centered = centered_ref[:, own]
        rows = jnp.concatenate(
            [(centered * scale[k : k + 1]).astype(BF) for k in range(4)], axis=0
        )
        shift2 = jnp.concatenate(halves(shift), axis=0)
        wq, wk = w_ref[0:256], w_ref[256:512]
        wv = twin(w_ref[512:640].astype(F32)).astype(BF)
        mq = mq + dot(rows, wq)
        mk = mk + dot(rows, wk)
        mv = mv + dot(rows, wv)
        for j, w in enumerate((wq, wk, wv)):
            b = dot(shift2, w)
            biases[j] = biases[j] + b[:4] + b[4:]
    line = lax.broadcasted_iota(jnp.int32, (16, LN), 0)
    low = low_lanes((32, LN))
    for k in range(4):
        at = slice(k * 64, k * 64 + 64)
        out_ref[k, 0:64] = mq[at].astype(BF)
        out_ref[k, 64:128] = mk[at].astype(BF)
        v = mv[at]
        out_ref[k, 128:160] = jnp.where(low, v[:32], v[32:]).astype(BF)
        tile = jnp.where(line == 0, biases[0][k : k + 1], 0.0)
        tile = jnp.where(line == 1, biases[1][k : k + 1], tile)
        tile = jnp.where(line == 2, biases[2][k : k + 1], tile)
        out_ref[k, 160:176] = tile.astype(BF)


def attend_kernel(parts_ref, lat_ref, gram_ref, out_ref):
    total = jnp.sum(parts_ref[...].astype(F32), axis=0)
    mq, mk, mv = total[0:64], total[64:128], total[128:160]
    mv = twin(mv)
    bias_q, bias_k, bias_v = total[160:161], total[161:162], total[162:163]
    packed = lat_ref[:, 0:16, :].reshape(512, LN)
    as_float = packed.astype(F32)
    square = (dot(packed, gram_ref[0]) + dot(packed, gram_ref[1])) * as_float
    low = low_lanes((512, LN))
    gain_low = lax.rsqrt(jnp.sum(jnp.where(low, square, 0.0), axis=1, keepdims=True) + 1e-06)
    gain_high = lax.rsqrt(jnp.sum(jnp.where(low, 0.0, square), axis=1, keepdims=True) + 1e-06)
    twice = jnp.concatenate([packed, packed], axis=1)
    none = jnp.zeros((64, LN), BF)

    def project(m, bias):
        hi, lo = halves(m)
        first = dot(twice, jnp.concatenate([hi, none, lo, none], axis=0))
        second = dot(twice, jnp.concatenate([none, hi, none, lo], axis=0))
        return gain_low * first + bias, gain_high * second + bias

    def unit(u, factor):
        mean = jnp.mean(u * u, axis=1, keepdims=True)
        return (u * (lax.rsqrt(mean + 1e-06) * factor)).astype(BF)

    q_low, q_high = (unit(u, math.log2(math.e) / math.sqrt(128)) for u in project(mq, bias_q))
    keys = jnp.concatenate([unit(u, 1.0) for u in project(mk, bias_k)], axis=0)
    values = jnp.concatenate(project(mv, bias_v), axis=0)
    all_low = low_lanes((1024, LN))
    values_low = jnp.where(all_low, values, 1.0).astype(BF)
    values_high = jnp.where(all_low, 1.0, values).astype(BF)

    def attend(q, v):
        return dot(jnp.exp2(dot_t(q, keys)).astype(BF), v)

    side = low_lanes((256, LN))
    for core in range(2):
        at = slice(core * 256, core * 256 + 256)
        first = attend(q_low[at], values_low)
        second = attend(q_high[at], values_high)
        over = jnp.where(side, first, second)
        under = pltpu.roll(jnp.where(side, second, first), LN // 2, 1)
        shares = (over / under).astype(BF)
        for z in range(8):
            out_ref[z * 2 + core] = shares[z * 32 : z * 32 + 32]


def step_of(stamps_ref, step):
    width = jnp.full((16, LN), stamps_ref[step + 1] - stamps_ref[step], jnp.int32)
    return width.astype(F32) / 1000.0


def increments_kernel(stamps_ref, shares_ref, lat_ref, out_ref, own_ref):
    step, side = place(*STEP), place("y_hi")
    velocity = jnp.sum(shares_ref[...].astype(F32), axis=0)
    size = step_of(stamps_ref, step)
    start = jnp.where(step == 0, pack_rows(lat_ref[0]), 0.0)
    for part in range(2):
        mine = velocity[part * 16 : part * 16 + 16]
        grown = size * mine
        grown = jnp.where(side == part, grown + start, grown).astype(BF)
        for peer in range(16):
            out_ref[peer * 2 + part] = grown
    own_ref[...] = jnp.where(side == 0, velocity[:16], velocity[16:])


def finish_kernel(stamps_ref, terms_ref, own_ref, lat_ref, updated_ref, velocity_ref):
    step, side = place(*STEP), place("y_hi")
    own = own_ref[...]
    size = step_of(stamps_ref, step)
    other = terms_ref[step * 2 + 1 - side].astype(F32)
    start = jnp.where(step == 0, pack_rows(lat_ref[0]), 0.0)
    velocity = own + other / size
    updated = size * own + start + other
    for j in range(15):
        term = terms_ref[2 * j].astype(F32) + terms_ref[2 * j + 1].astype(F32)
        updated = updated + jnp.where(j < step, term, 0.0)
    for ref, value in ((updated_ref, updated), (velocity_ref, velocity)):
        ref[0, 0:16] = value[:, : LN // 2]
        ref[0, 16:32] = pltpu.roll(value, LN // 2, 1)[:, : LN // 2]


def over_x(w, far):
    return lax.ppermute(w, "x", [(i, (i + far) % 4) for i in range(4)])


def near(x):
    return pltpu.with_memory_space_constraint(x, pltpu.VMEM)


def call(kernel, outs, *args, scalars=(), scratch=()):
    smem = pl.BlockSpec(memory_space=pltpu.SMEM)
    vmem = pl.BlockSpec(memory_space=pltpu.VMEM)
    return pl.pallas_call(
        kernel,
        in_specs=[smem] * len(scalars) + [vmem] * len(args),
        out_specs=[vmem] * len(outs),
        out_shape=outs,
        scratch_shapes=scratch,
    )(*scalars, *args)


def stages(latents, timesteps, embed_weight, mod_weight, qkv_weight, out_weight):
    vmem = pltpu.VMEM
    payload, w = call(
        pack_kernel,
        [vmem((16, 80, LN), BF), vmem((640, LN), BF)],
        latents,
        mod_weight,
        jnp.moveaxis(qkv_weight[:, 0], 1, 0),
        jnp.swapaxes(out_weight, 1, 2),
        scalars=(timesteps,),
    )
    payload = lax.all_to_all(payload, ("z", "y_hi"), 0, 0, tiled=True)
    gathered = near(lax.all_gather(payload, "core", tiled=True))
    ws = {2: over_x(w, 2)}
    ws.update({far: over_x(w, far) for far in (1, 3)})
    centered, gram = call(
        weights_kernel, [vmem((64, 1024), F32), vmem((2, LN, LN), BF)], near(embed_weight)
    )
    (parts,) = call(
        partial_kernel,
        [vmem((4, 176, LN), BF)],
        gathered,
        near(centered),
        near(w),
        *[near(ws[far]) for far in (1, 2, 3)],
        scratch=[vmem((8, 1024), F32)],
    )
    parts = near(lax.all_to_all(parts, "y_lo", 0, 0, tiled=True))
    (shares,) = call(attend_kernel, [vmem((16, 32, LN), BF)], parts, gathered, near(gram))
    shares = near(lax.all_to_all(shares, ("z", "core"), 0, 0, tiled=True))
    terms, own = call(
        increments_kernel,
        [vmem((32, 16, LN), BF), vmem((16, LN), F32)],
        shares,
        near(latents),
        scalars=(timesteps,),
    )
    terms = near(lax.all_to_all(terms, ("y_lo", "x", "y_hi"), 0, 0, tiled=True))
    out = jax.ShapeDtypeStruct(latents.shape, F32)
    return tuple(
        call(finish_kernel, [out, out], terms, near(own), near(latents), scalars=(timesteps,))
    )


def solution(mesh):
    split = Mesh(mesh.devices.reshape(4, 4, 8, 2, 2), STEP + SEQ)
    return jax.shard_map(
        stages,
        mesh=split,
        in_specs=(
            P(STEP, SEQ, None),
            P(),
            P(),
            P(SEQ, None, None),
            P(STEP, SEQ, None, None),
            P(SEQ, None, None),
        ),
        out_specs=(P(STEP, SEQ, None), P(STEP, SEQ, None)),
        check_vma=False,
    )
```

```python
import math

import jax
import jax.numpy as jnp
from jax import lax
from jax.experimental import pallas as pl
from jax.experimental.pallas import tpu as pltpu
from jax.sharding import Mesh
from jax.sharding import PartitionSpec as P


STEP = ("y_lo", "x")
SEQ = ("z", "y_hi", "core")
BF = jnp.bfloat16
F32 = jnp.float32
LN = 128


def dot(a, b):
    return jnp.dot(a, b, preferred_element_type=F32)


def dot_t(a, b):
    return lax.dot_general(a, b, (((1,), (1,)), ((), ())), preferred_element_type=F32)


def halves(x):
    hi = x.astype(BF)
    return hi, (x - hi.astype(F32)).astype(BF)


def low_lanes(shape):
    return lax.broadcasted_iota(jnp.int32, shape, len(shape) - 1) < LN // 2


def pack_rows(rows):
    return jnp.concatenate([rows[:16], rows[16:]], axis=1)


def place(*axes):
    index = 0
    for axis in axes:
        index = index * lax.axis_size(axis) + lax.axis_index(axis)
    return index


def own_columns():
    return pl.ds(pl.multiple_of(place("y_lo") * 1024, 1024), 1024)


def conditions(stamps_ref):
    shape = (8, 16)
    row = lax.broadcasted_iota(jnp.int32, shape, 0)
    col = lax.broadcasted_iota(jnp.int32, shape, 1)
    stamp = jnp.zeros(shape, jnp.int32)
    for k in range(4):
        stamp = jnp.where(row % 4 == k, stamps_ref[k * 4 + place("x")], stamp)
    feature = place(*SEQ) * 8 + col % 8
    half_count = 128
    frequencies = jnp.exp(-math.log(10000.0) * (feature % half_count).astype(F32) / half_count)
    angles = stamp.astype(F32) * frequencies
    value = jnp.where(feature < half_count, jnp.cos(angles), jnp.sin(angles))
    return jnp.where(row // 4 == col // 8, value, 0.0)


def twin(lines):
    low = low_lanes(lines.shape)
    turned = pltpu.roll(lines, LN // 2, 1)
    return jnp.concatenate([jnp.where(low, lines, turned), jnp.where(low, turned, lines)], axis=0)


def pack_kernel(stamps_ref, lat_ref, mw_ref, w_ref, out_weight_ref, out_ref, folded_ref):
    out = out_weight_ref[0]
    wv = dot_t(w_ref[2], jnp.concatenate([out, out], axis=0))
    folded_ref[0:512] = w_ref[0:2].reshape(512, LN)
    folded_ref[512:640] = jnp.where(low_lanes((LN, LN)), wv[:LN], wv[LN:]).astype(BF)
    lat = pack_rows(lat_ref[0]).astype(BF)
    own = own_columns()
    cond_hi, cond_lo = halves(conditions(stamps_ref))
    hi, lo = halves(jnp.concatenate([mw_ref[:, 0, own], mw_ref[:, 1, own]], axis=0))
    share = dot(cond_hi, hi) + dot(cond_lo, hi) + dot(cond_hi, lo)
    blocks = [share[:, part * LN : (part + 1) * LN] for part in range(8)]
    payload = jnp.concatenate([lat, jnp.concatenate(blocks, axis=0).astype(BF)], axis=0)
    for peer in range(out_ref.shape[0]):
        out_ref[peer] = payload


def weights_kernel(embed_ref, centered_ref, gram_ref):
    embed = embed_ref[...].astype(F32)
    mean = jnp.mean(embed, axis=1, keepdims=True)
    centered_ref[...] = embed_ref[:, own_columns()].astype(F32) - mean
    hi, lo = halves(embed - mean)
    products = dot_t(jnp.concatenate([hi, lo], axis=0), hi)
    cross = products[64:]
    gram = (products[:64] + cross + cross.T) * (1.0 / embed.shape[1])
    none = jnp.zeros_like(gram)
    gram = jnp.concatenate(
        [jnp.concatenate([gram, none], axis=1), jnp.concatenate([none, gram], axis=1)], axis=0
    )
    gram_ref[0], gram_ref[1] = halves(gram)


def partial_kernel(mod_ref, centered_ref, *refs):
    w_refs, out_ref, modulation_ref = refs[:4], refs[4], refs[5]
    total = jnp.sum(mod_ref[:, 16:80, :].astype(F32), axis=0)
    for part in range(8):
        modulation_ref[:, part * LN : (part + 1) * LN] = total[part * 8 : part * 8 + 8]
    m_qk = m_v = 0.0
    for far, w_ref in enumerate(w_refs):
        origin = lax.rem(place("x") + 4 - far, 4)
        own = pl.ds(pl.multiple_of(origin * 256, 256), 256)
        modulation = modulation_ref[:, own]
        shift, scale = modulation[:4], modulation[4:]
        centered = centered_ref[:, own]
        scaled = [(centered * scale[k : k + 1]).astype(BF) for k in range(4)]
        shifts = jnp.concatenate([*halves(shift), jnp.zeros((8, 256), BF)], axis=0)
        rows = jnp.concatenate([*halves(centered), *scaled, shifts], axis=0)
        m_qk = m_qk + dot(rows, jnp.concatenate([w_ref[0:256], w_ref[256:512]], axis=1))
        m_v = m_v + dot(rows, twin(w_ref[512:640].astype(F32)).astype(BF))
    line = lax.broadcasted_iota(jnp.int32, (16, LN), 0)
    low = low_lanes((32, LN))
    plain_qk = m_qk[0:64] + m_qk[64:128]
    plain_v = m_v[0:64] + m_v[64:128]
    for k in range(4):
        at = slice(128 + k * 64, 192 + k * 64)
        qk = plain_qk + m_qk[at]
        v = plain_v + m_v[at]
        out_ref[k, 0:64] = qk[:, :LN].astype(BF)
        out_ref[k, 64:128] = qk[:, LN:].astype(BF)
        out_ref[k, 128:160] = jnp.where(low, v[:32], v[32:]).astype(BF)
        hi, lo = slice(384 + k, 385 + k), slice(388 + k, 389 + k)
        b_qk, b_v = m_qk[hi] + m_qk[lo], m_v[hi] + m_v[lo]
        tile = jnp.where(line == 0, b_qk[:, :LN], 0.0)
        tile = jnp.where(line == 1, b_qk[:, LN:], tile)
        tile = jnp.where(line == 2, b_v, tile)
        out_ref[k, 160:176] = tile.astype(BF)


def attend_kernel(parts_ref, lat_ref, gram_ref, out_ref):
    total = jnp.sum(parts_ref[...].astype(F32), axis=0)
    mq, mk, mv = total[0:64], total[64:128], total[128:160]
    mv = twin(mv)
    bias_q, bias_k, bias_v = total[160:161], total[161:162], total[162:163]
    packed = lat_ref[:, 0:16, :].reshape(512, LN)
    as_float = packed.astype(F32)
    twice = jnp.concatenate([packed, packed], axis=1)
    square = dot(twice, gram_ref[...].reshape(256, LN)) * as_float
    low = low_lanes((512, LN))
    gain_low = lax.rsqrt(jnp.sum(jnp.where(low, square, 0.0), axis=1, keepdims=True) + 1e-06)
    gain_high = lax.rsqrt(jnp.sum(jnp.where(low, 0.0, square), axis=1, keepdims=True) + 1e-06)
    none = jnp.zeros((64, 2 * LN), BF)
    hi, lo = halves(jnp.concatenate([mq, mk], axis=1))
    qk_low = gain_low * dot(twice, jnp.concatenate([hi, none, lo, none], axis=0))
    qk_high = gain_high * dot(twice, jnp.concatenate([none, hi, none, lo], axis=0))
    hi, lo = halves(mv)
    none = jnp.zeros((64, LN), BF)
    for_low = jnp.concatenate([hi, none, lo, none], axis=0)
    for_high = jnp.concatenate([none, hi, none, lo], axis=0)
    v_both = dot(twice, jnp.concatenate([for_low, for_high], axis=1))

    def unit(u, factor):
        mean = jnp.mean(u * u, axis=1, keepdims=True)
        return (u * (lax.rsqrt(mean + 1e-06) * factor)).astype(BF)

    factor = math.log2(math.e) / math.sqrt(128)
    q_low, q_high = (unit(u[:, :LN] + bias_q, factor) for u in (qk_low, qk_high))
    keys = jnp.concatenate([unit(u[:, LN:] + bias_k, 1.0) for u in (qk_low, qk_high)], axis=0)
    values = (
        jnp.concatenate([gain_low * v_both[:, :LN], gain_high * v_both[:, LN:]], axis=0) + bias_v
    )
    all_low = low_lanes((1024, LN))
    values_low = jnp.where(all_low, values, 1.0).astype(BF)
    values_high = jnp.where(all_low, 1.0, values).astype(BF)

    def attend(q, v):
        return dot(jnp.exp2(dot_t(q, keys)).astype(BF), v)

    side = low_lanes((256, LN))
    for core in range(2):
        at = slice(core * 256, core * 256 + 256)
        first = attend(q_low[at], values_low)
        second = attend(q_high[at], values_high)
        over = jnp.where(side, first, second)
        under = pltpu.roll(jnp.where(side, second, first), LN // 2, 1)
        shares = (over / under).astype(BF)
        for z in range(8):
            out_ref[z * 2 + core] = shares[z * 32 : z * 32 + 32]


def step_of(stamps_ref, step):
    width = jnp.full((16, LN), stamps_ref[step + 1] - stamps_ref[step], jnp.int32)
    return width.astype(F32) / 1000.0


def increments_kernel(stamps_ref, shares_ref, lat_ref, out_ref, own_ref):
    step, side = place(*STEP), place("y_hi")
    velocity = jnp.sum(shares_ref[...].astype(F32), axis=0)
    size = step_of(stamps_ref, step)
    start = jnp.where(step == 0, pack_rows(lat_ref[0]), 0.0)
    for part in range(2):
        mine = velocity[part * 16 : part * 16 + 16]
        grown = size * mine
        grown = jnp.where(side == part, grown + start, grown).astype(BF)
        for peer in range(16):
            out_ref[peer * 2 + part] = grown
    own_ref[...] = jnp.where(side == 0, velocity[:16], velocity[16:])


def finish_kernel(stamps_ref, terms_ref, own_ref, lat_ref, updated_ref, velocity_ref):
    step, side = place(*STEP), place("y_hi")
    own = own_ref[...]
    size = step_of(stamps_ref, step)
    other = terms_ref[step * 2 + 1 - side].astype(F32)
    start = jnp.where(step == 0, pack_rows(lat_ref[0]), 0.0)
    velocity = own + other / size
    updated = size * own + start + other
    for j in range(15):
        term = terms_ref[2 * j].astype(F32) + terms_ref[2 * j + 1].astype(F32)
        updated = updated + jnp.where(j < step, term, 0.0)
    for ref, value in ((updated_ref, updated), (velocity_ref, velocity)):
        ref[0, 0:16] = value[:, : LN // 2]
        ref[0, 16:32] = pltpu.roll(value, LN // 2, 1)[:, : LN // 2]


def over_x(w, far):
    return lax.ppermute(w, "x", [(i, (i + far) % 4) for i in range(4)])


def near(x):
    return pltpu.with_memory_space_constraint(x, pltpu.VMEM)


def call(kernel, outs, *args, scalars=(), scratch=()):
    smem = pl.BlockSpec(memory_space=pltpu.SMEM)
    vmem = pl.BlockSpec(memory_space=pltpu.VMEM)
    return pl.pallas_call(
        kernel,
        in_specs=[smem] * len(scalars) + [vmem] * len(args),
        out_specs=[vmem] * len(outs),
        out_shape=outs,
        scratch_shapes=scratch,
    )(*scalars, *args)


def stages(latents, timesteps, embed_weight, mod_weight, qkv_weight, out_weight):
    vmem = pltpu.VMEM
    payload, w = call(
        pack_kernel,
        [vmem((16, 80, LN), BF), vmem((640, LN), BF)],
        latents,
        mod_weight,
        jnp.moveaxis(qkv_weight[:, 0], 1, 0),
        jnp.swapaxes(out_weight, 1, 2),
        scalars=(timesteps,),
    )
    payload = lax.all_to_all(payload, ("z", "y_hi"), 0, 0, tiled=True)
    gathered = near(lax.all_gather(payload, "core", tiled=True))
    ws = {2: over_x(w, 2)}
    ws.update({far: over_x(w, far) for far in (1, 3)})
    centered, gram = call(
        weights_kernel, [vmem((64, 1024), F32), vmem((2, LN, LN), BF)], near(embed_weight)
    )
    (parts,) = call(
        partial_kernel,
        [vmem((4, 176, LN), BF)],
        gathered,
        near(centered),
        near(w),
        *[near(ws[far]) for far in (1, 2, 3)],
        scratch=[vmem((8, 1024), F32)],
    )
    parts = near(lax.all_to_all(parts, "y_lo", 0, 0, tiled=True))
    (shares,) = call(attend_kernel, [vmem((16, 32, LN), BF)], parts, gathered, near(gram))
    shares = near(lax.all_to_all(shares, ("z", "core"), 0, 0, tiled=True))
    terms, own = call(
        increments_kernel,
        [vmem((32, 16, LN), BF), vmem((16, LN), F32)],
        shares,
        near(latents),
        scalars=(timesteps,),
    )
    terms = near(lax.all_to_all(terms, ("y_lo", "x", "y_hi"), 0, 0, tiled=True))
    out = jax.ShapeDtypeStruct(latents.shape, F32)
    return tuple(
        call(finish_kernel, [out, out], terms, near(own), near(latents), scalars=(timesteps,))
    )


def solution(mesh):
    split = Mesh(mesh.devices.reshape(4, 4, 8, 2, 2), STEP + SEQ)
    return jax.shard_map(
        stages,
        mesh=split,
        in_specs=(
            P(STEP, SEQ, None),
            P(),
            P(),
            P(SEQ, None, None),
            P(STEP, SEQ, None, None),
            P(SEQ, None, None),
        ),
        out_specs=(P(STEP, SEQ, None), P(STEP, SEQ, None)),
        check_vma=False,
    )
```

```python
import math

import jax
import jax.numpy as jnp
from jax import lax
from jax.experimental import pallas as pl
from jax.experimental.pallas import tpu as pltpu
from jax.sharding import Mesh
from jax.sharding import PartitionSpec as P


STEP = ("y_lo", "x")
SEQ = ("z", "y_hi", "core")
BF = jnp.bfloat16
F32 = jnp.float32
LN = 128


def dot(a, b):
    return jnp.dot(a, b, preferred_element_type=F32)


def dot_t(a, b):
    return lax.dot_general(a, b, (((1,), (1,)), ((), ())), preferred_element_type=F32)


def halves(x):
    hi = x.astype(BF)
    return hi, (x - hi.astype(F32)).astype(BF)


def low_lanes(shape):
    return lax.broadcasted_iota(jnp.int32, shape, len(shape) - 1) < LN // 2


def pack_rows(rows):
    return jnp.concatenate([rows[:16], rows[16:]], axis=1)


def place(*axes):
    index = 0
    for axis in axes:
        index = index * lax.axis_size(axis) + lax.axis_index(axis)
    return index


def own_columns():
    return pl.ds(pl.multiple_of(place("y_lo") * 1024, 1024), 1024)


def conditions(stamps_ref):
    shape = (8, 16)
    row = lax.broadcasted_iota(jnp.int32, shape, 0)
    col = lax.broadcasted_iota(jnp.int32, shape, 1)
    stamp = jnp.zeros(shape, jnp.int32)
    for k in range(4):
        stamp = jnp.where(row % 4 == k, stamps_ref[k * 4 + place("x")], stamp)
    feature = place(*SEQ) * 8 + col % 8
    half_count = 128
    frequencies = jnp.exp(-math.log(10000.0) * (feature % half_count).astype(F32) / half_count)
    angles = stamp.astype(F32) * frequencies
    value = jnp.where(feature < half_count, jnp.cos(angles), jnp.sin(angles))
    return jnp.where(row // 4 == col // 8, value, 0.0)


def twin(lines):
    low = low_lanes(lines.shape)
    turned = pltpu.roll(lines, LN // 2, 1)
    return jnp.concatenate([jnp.where(low, lines, turned), jnp.where(low, turned, lines)], axis=0)


def pack_kernel(stamps_ref, lat_ref, mw_ref, w_ref, out_weight_ref, out_ref, folded_ref):
    out = out_weight_ref[0]
    wv = dot_t(w_ref[2], jnp.concatenate([out, out], axis=0))
    folded_ref[0:512] = w_ref[0:2].reshape(512, LN)
    folded_ref[512:640] = jnp.where(low_lanes((LN, LN)), wv[:LN], wv[LN:]).astype(BF)
    lat = pack_rows(lat_ref[0]).astype(BF)
    own = own_columns()
    cond_hi, cond_lo = halves(conditions(stamps_ref))
    hi, lo = halves(jnp.concatenate([mw_ref[:, 0, own], mw_ref[:, 1, own]], axis=0))
    share = dot(cond_hi, hi) + dot(cond_lo, hi) + dot(cond_hi, lo)
    blocks = [share[:, part * LN : (part + 1) * LN] for part in range(8)]
    payload = jnp.concatenate([lat, jnp.concatenate(blocks, axis=0).astype(BF)], axis=0)
    for peer in range(out_ref.shape[0]):
        out_ref[peer] = payload


def weights_kernel(embed_ref, _, centered_ref, gram_ref):
    embed = embed_ref[...].astype(F32)
    mean = jnp.mean(embed, axis=1, keepdims=True)
    centered_ref[...] = embed_ref[:, own_columns()].astype(F32) - mean
    hi, lo = halves(embed - mean)
    products = dot_t(jnp.concatenate([hi, lo], axis=0), hi)
    cross = products[64:]
    gram = (products[:64] + cross + cross.T) * (1.0 / embed.shape[1])
    none = jnp.zeros_like(gram)
    gram = jnp.concatenate(
        [jnp.concatenate([gram, none], axis=1), jnp.concatenate([none, gram], axis=1)], axis=0
    )
    gram_ref[0], gram_ref[1] = halves(gram)


def partial_kernel(mod_ref, centered_ref, *refs):
    w_refs, out_ref, modulation_ref = refs[:4], refs[4], refs[5]
    total = jnp.sum(mod_ref[:, 16:80, :].astype(F32), axis=0)
    for part in range(8):
        modulation_ref[:, part * LN : (part + 1) * LN] = total[part * 8 : part * 8 + 8]
    m_qk = m_v = 0.0
    for far, w_ref in enumerate(w_refs):
        origin = lax.rem(place("x") + 4 - far, 4)
        own = pl.ds(pl.multiple_of(origin * 256, 256), 256)
        modulation = modulation_ref[:, own]
        shift, scale = modulation[:4], modulation[4:]
        centered = centered_ref[:, own]
        scaled = [(centered * scale[k : k + 1]).astype(BF) for k in range(4)]
        shifts = jnp.concatenate([*halves(shift), jnp.zeros((8, 256), BF)], axis=0)
        rows = jnp.concatenate([*halves(centered), *scaled, shifts], axis=0)
        m_qk = m_qk + dot(rows, jnp.concatenate([w_ref[0:256], w_ref[256:512]], axis=1))
        m_v = m_v + dot(rows, twin(w_ref[512:640].astype(F32)).astype(BF))
    line = lax.broadcasted_iota(jnp.int32, (16, LN), 0)
    low = low_lanes((32, LN))
    plain_qk = m_qk[0:64] + m_qk[64:128]
    plain_v = m_v[0:64] + m_v[64:128]
    for k in range(4):
        at = slice(128 + k * 64, 192 + k * 64)
        qk = plain_qk + m_qk[at]
        v = plain_v + m_v[at]
        out_ref[k, 0:64] = qk[:, :LN].astype(BF)
        out_ref[k, 64:128] = qk[:, LN:].astype(BF)
        out_ref[k, 128:160] = jnp.where(low, v[:32], v[32:]).astype(BF)
        hi, lo = slice(384 + k, 385 + k), slice(388 + k, 389 + k)
        b_qk, b_v = m_qk[hi] + m_qk[lo], m_v[hi] + m_v[lo]
        tile = jnp.zeros((16, LN), F32)
        for i, bias in enumerate((b_qk[:, :LN], b_qk[:, LN:], b_v)):
            rounded = bias.astype(BF).astype(F32)
            tile = jnp.where(line == i, rounded, tile)
            tile = jnp.where(line == i + 3, bias - rounded, tile)
        out_ref[k, 160:176] = tile.astype(BF)


def attend_kernel(parts_ref, lat_ref, gram_ref, out_ref):
    total = jnp.sum(parts_ref[...].astype(F32), axis=0)
    mq, mk, mv = total[0:64], total[64:128], total[128:160]
    mv = twin(mv)
    bias_q, bias_k, bias_v = (total[i : i + 1] + total[i + 3 : i + 4] for i in (160, 161, 162))
    packed = lat_ref[:, 0:16, :].reshape(512, LN)
    as_float = packed.astype(F32)
    twice = jnp.concatenate([packed, packed], axis=1)
    square = dot(twice, gram_ref[...].reshape(256, LN)) * as_float
    low = low_lanes((512, LN))
    gain_low = lax.rsqrt(jnp.sum(jnp.where(low, square, 0.0), axis=1, keepdims=True) + 1e-06)
    gain_high = lax.rsqrt(jnp.sum(jnp.where(low, 0.0, square), axis=1, keepdims=True) + 1e-06)
    none = jnp.zeros((64, 2 * LN), BF)
    hi, lo = halves(jnp.concatenate([mq, mk], axis=1))
    qk_low = gain_low * dot(twice, jnp.concatenate([hi, none, lo, none], axis=0))
    qk_high = gain_high * dot(twice, jnp.concatenate([none, hi, none, lo], axis=0))
    hi, lo = halves(mv)
    none = jnp.zeros((64, LN), BF)
    for_low = jnp.concatenate([hi, none, lo, none], axis=0)
    for_high = jnp.concatenate([none, hi, none, lo], axis=0)
    v_both = dot(twice, jnp.concatenate([for_low, for_high], axis=1))

    def unit(u, factor):
        mean = jnp.mean(u * u, axis=1, keepdims=True)
        return (u * (lax.rsqrt(mean + 1e-06) * factor)).astype(BF)

    factor = math.log2(math.e) / math.sqrt(128)
    q_low, q_high = (unit(u[:, :LN] + bias_q, factor) for u in (qk_low, qk_high))
    keys = jnp.concatenate([unit(u[:, LN:] + bias_k, 1.0) for u in (qk_low, qk_high)], axis=0)
    values = (
        jnp.concatenate([gain_low * v_both[:, :LN], gain_high * v_both[:, LN:]], axis=0) + bias_v
    )
    all_low = low_lanes((1024, LN))
    values_low = jnp.where(all_low, values, 1.0).astype(BF)
    values_high = jnp.where(all_low, 1.0, values).astype(BF)

    def attend(q, v):
        return dot(jnp.exp2(dot_t(q, keys)).astype(BF), v)

    side = low_lanes((256, LN))
    for core in range(2):
        at = slice(core * 256, core * 256 + 256)
        first = attend(q_low[at], values_low)
        second = attend(q_high[at], values_high)
        over = jnp.where(side, first, second)
        under = pltpu.roll(jnp.where(side, second, first), LN // 2, 1)
        shares = (over / under).astype(BF)
        for z in range(8):
            out_ref[z * 2 + core] = shares[z * 32 : z * 32 + 32]


def step_of(stamps_ref, step):
    width = jnp.full((16, LN), stamps_ref[step + 1] - stamps_ref[step], jnp.int32)
    return width.astype(F32) / 1000.0


def increments_kernel(stamps_ref, shares_ref, lat_ref, out_ref, own_ref):
    step, side = place(*STEP), place("y_hi")
    velocity = jnp.sum(shares_ref[...].astype(F32), axis=0)
    size = step_of(stamps_ref, step)
    start = jnp.where(step == 0, pack_rows(lat_ref[0]), 0.0)
    for part in range(2):
        mine = velocity[part * 16 : part * 16 + 16]
        grown = size * mine
        grown = jnp.where(side == part, grown + start, grown).astype(BF)
        for peer in range(16):
            out_ref[peer * 2 + part] = grown
    own_ref[...] = jnp.where(side == 0, velocity[:16], velocity[16:])


def finish_kernel(stamps_ref, terms_ref, own_ref, lat_ref, updated_ref, velocity_ref):
    step, side = place(*STEP), place("y_hi")
    own = own_ref[...]
    size = step_of(stamps_ref, step)
    other = terms_ref[step * 2 + 1 - side].astype(F32)
    start = jnp.where(step == 0, pack_rows(lat_ref[0]), 0.0)
    velocity = own + other / size
    updated = size * own + start + other
    for j in range(15):
        term = terms_ref[2 * j].astype(F32) + terms_ref[2 * j + 1].astype(F32)
        updated = updated + jnp.where(j < step, term, 0.0)
    for ref, value in ((updated_ref, updated), (velocity_ref, velocity)):
        ref[0, 0:16] = value[:, : LN // 2]
        ref[0, 16:32] = pltpu.roll(value, LN // 2, 1)[:, : LN // 2]


def over_x(w, far):
    return lax.ppermute(w, "x", [(i, (i + far) % 4) for i in range(4)])


def near(x):
    return pltpu.with_memory_space_constraint(x, pltpu.VMEM)


def call(kernel, outs, *args, scalars=(), scratch=()):
    smem = pl.BlockSpec(memory_space=pltpu.SMEM)
    vmem = pl.BlockSpec(memory_space=pltpu.VMEM)
    return pl.pallas_call(
        kernel,
        in_specs=[smem] * len(scalars) + [vmem] * len(args),
        out_specs=[vmem] * len(outs),
        out_shape=outs,
        scratch_shapes=scratch,
    )(*scalars, *args)


def stages(latents, timesteps, embed_weight, mod_weight, qkv_weight, out_weight):
    vmem = pltpu.VMEM
    payload, w = call(
        pack_kernel,
        [vmem((16, 80, LN), BF), vmem((640, LN), BF)],
        latents,
        mod_weight,
        jnp.moveaxis(qkv_weight[:, 0], 1, 0),
        jnp.swapaxes(out_weight, 1, 2),
        scalars=(timesteps,),
    )
    payload = lax.all_to_all(payload, ("z", "y_hi"), 0, 0, tiled=True)
    gathered = near(lax.all_gather(payload, "core", tiled=True))
    ws = {2: over_x(w, 2)}
    ws.update({far: over_x(w, far) for far in (1, 3)})
    centered, gram = call(
        weights_kernel, [vmem((64, 1024), F32), vmem((2, LN, LN), BF)], near(embed_weight), gathered
    )
    (parts,) = call(
        partial_kernel,
        [vmem((4, 176, LN), BF)],
        gathered,
        near(centered),
        near(w),
        *[near(ws[far]) for far in (1, 2, 3)],
        scratch=[vmem((8, 1024), F32)],
    )
    parts = near(lax.all_to_all(parts, "y_lo", 0, 0, tiled=True))
    (shares,) = call(attend_kernel, [vmem((16, 32, LN), BF)], parts, gathered, near(gram))
    shares = near(lax.all_to_all(shares, ("z", "core"), 0, 0, tiled=True))
    terms, own = call(
        increments_kernel,
        [vmem((32, 16, LN), BF), vmem((16, LN), F32)],
        shares,
        near(latents),
        scalars=(timesteps,),
    )
    terms = near(lax.all_to_all(terms, ("y_lo", "x", "y_hi"), 0, 0, tiled=True))
    out = jax.ShapeDtypeStruct(latents.shape, F32)
    return tuple(
        call(finish_kernel, [out, out], terms, near(own), near(latents), scalars=(timesteps,))
    )


def solution(mesh):
    split = Mesh(mesh.devices.reshape(4, 4, 8, 2, 2), STEP + SEQ)
    return jax.shard_map(
        stages,
        mesh=split,
        in_specs=(
            P(STEP, SEQ, None),
            P(),
            P(),
            P(SEQ, None, None),
            P(STEP, SEQ, None, None),
            P(SEQ, None, None),
        ),
        out_specs=(P(STEP, SEQ, None), P(STEP, SEQ, None)),
        check_vma=False,
    )
```

```python
import math

import jax
import jax.numpy as jnp
from jax import lax
from jax.experimental import pallas as pl
from jax.experimental.pallas import tpu as pltpu
from jax.sharding import Mesh
from jax.sharding import PartitionSpec as P


STEP = ("y_lo", "x")
SEQ = ("z", "y_hi", "core")
BF = jnp.bfloat16
F32 = jnp.float32
LN = 128


def dot(a, b):
    return jnp.dot(a, b, preferred_element_type=F32)


def dot_t(a, b):
    return lax.dot_general(a, b, (((1,), (1,)), ((), ())), preferred_element_type=F32)


def halves(x):
    hi = x.astype(BF)
    return hi, (x - hi.astype(F32)).astype(BF)


def low_lanes(shape):
    return lax.broadcasted_iota(jnp.int32, shape, len(shape) - 1) < LN // 2


def pack_rows(rows):
    return jnp.concatenate([rows[:16], rows[16:]], axis=1)


def place(*axes):
    index = 0
    for axis in axes:
        index = index * lax.axis_size(axis) + lax.axis_index(axis)
    return index


def own_columns():
    return pl.ds(pl.multiple_of(place("y_lo") * 1024, 1024), 1024)


def conditions(stamps_ref):
    shape = (8, 16)
    row = lax.broadcasted_iota(jnp.int32, shape, 0)
    col = lax.broadcasted_iota(jnp.int32, shape, 1)
    stamp = jnp.zeros(shape, jnp.int32)
    for k in range(4):
        stamp = jnp.where(row % 4 == k, stamps_ref[k * 4 + place("x")], stamp)
    feature = place(*SEQ) * 8 + col % 8
    half_count = 128
    frequencies = jnp.exp(-math.log(10000.0) * (feature % half_count).astype(F32) / half_count)
    angles = stamp.astype(F32) * frequencies
    value = jnp.where(feature < half_count, jnp.cos(angles), jnp.sin(angles))
    return jnp.where(row // 4 == col // 8, value, 0.0)


def twin(lines):
    low = low_lanes(lines.shape)
    turned = pltpu.roll(lines, LN // 2, 1)
    return jnp.concatenate([jnp.where(low, lines, turned), jnp.where(low, turned, lines)], axis=0)


def pack_kernel(stamps_ref, lat_ref, mw_ref, w_ref, out_weight_ref, out_ref, folded_ref, size_ref):
    size_ref[...] = step_of(stamps_ref, place(*STEP))
    out = out_weight_ref[0]
    wv = dot_t(w_ref[2], jnp.concatenate([out, out], axis=0))
    folded_ref[0:512] = w_ref[0:2].reshape(512, LN)
    folded_ref[512:640] = jnp.where(low_lanes((LN, LN)), wv[:LN], wv[LN:]).astype(BF)
    lat = pack_rows(lat_ref[0]).astype(BF)
    own = own_columns()
    cond_hi, cond_lo = halves(conditions(stamps_ref))
    hi, lo = halves(jnp.concatenate([mw_ref[:, 0, own], mw_ref[:, 1, own]], axis=0))
    share = dot(cond_hi, hi) + dot(cond_lo, hi) + dot(cond_hi, lo)
    blocks = [share[:, part * LN : (part + 1) * LN] for part in range(8)]
    payload = jnp.concatenate([lat, jnp.concatenate(blocks, axis=0).astype(BF)], axis=0)
    for peer in range(out_ref.shape[0]):
        out_ref[peer] = payload


def weights_kernel(embed_ref, _, centered_ref, gram_ref):
    embed = embed_ref[...].astype(F32)
    mean = jnp.mean(embed, axis=1, keepdims=True)
    centered_ref[...] = embed_ref[:, own_columns()].astype(F32) - mean
    hi, lo = halves(embed - mean)
    products = dot_t(jnp.concatenate([hi, lo], axis=0), hi)
    cross = products[64:]
    gram = (products[:64] + cross + cross.T) * (1.0 / embed.shape[1])
    none = jnp.zeros_like(gram)
    gram = jnp.concatenate(
        [jnp.concatenate([gram, none], axis=1), jnp.concatenate([none, gram], axis=1)], axis=0
    )
    gram_ref[0], gram_ref[1] = halves(gram)


def partial_kernel(mod_ref, centered_ref, *refs):
    w_refs, out_ref, modulation_ref = refs[:4], refs[4], refs[5]
    total = jnp.sum(mod_ref[:, 16:80, :].astype(F32), axis=0)
    for part in range(8):
        modulation_ref[:, part * LN : (part + 1) * LN] = total[part * 8 : part * 8 + 8]
    m_qk = m_v = 0.0
    for far, w_ref in enumerate(w_refs):
        origin = lax.rem(place("x") + 4 - far, 4)
        own = pl.ds(pl.multiple_of(origin * 256, 256), 256)
        modulation = modulation_ref[:, own]
        shift, scale = modulation[:4], modulation[4:]
        centered = centered_ref[:, own]
        scaled = [(centered * scale[k : k + 1]).astype(BF) for k in range(4)]
        shifts = jnp.concatenate([*halves(shift), jnp.zeros((8, 256), BF)], axis=0)
        rows = jnp.concatenate([*halves(centered), *scaled, shifts], axis=0)
        m_qk = m_qk + dot(rows, jnp.concatenate([w_ref[0:256], w_ref[256:512]], axis=1))
        m_v = m_v + dot(rows, twin(w_ref[512:640].astype(F32)).astype(BF))
    line = lax.broadcasted_iota(jnp.int32, (16, LN), 0)
    low = low_lanes((32, LN))
    plain_qk = m_qk[0:64] + m_qk[64:128]
    plain_v = m_v[0:64] + m_v[64:128]
    for k in range(4):
        at = slice(128 + k * 64, 192 + k * 64)
        qk = plain_qk + m_qk[at]
        v = plain_v + m_v[at]
        out_ref[k, 0:64] = qk[:, :LN].astype(BF)
        out_ref[k, 64:128] = qk[:, LN:].astype(BF)
        out_ref[k, 128:160] = jnp.where(low, v[:32], v[32:]).astype(BF)
        hi, lo = slice(384 + k, 385 + k), slice(388 + k, 389 + k)
        b_qk, b_v = m_qk[hi] + m_qk[lo], m_v[hi] + m_v[lo]
        tile = jnp.zeros((16, LN), F32)
        for i, bias in enumerate((b_qk[:, :LN], b_qk[:, LN:], b_v)):
            rounded = bias.astype(BF).astype(F32)
            tile = jnp.where(line == i, rounded, tile)
            tile = jnp.where(line == i + 3, bias - rounded, tile)
        out_ref[k, 160:176] = tile.astype(BF)


def attend_kernel(parts_ref, lat_ref, gram_ref, out_ref):
    total = jnp.sum(parts_ref[...].astype(F32), axis=0)
    mq, mk, mv = total[0:64], total[64:128], total[128:160]
    mv = twin(mv)
    bias_q, bias_k, bias_v = (total[i : i + 1] + total[i + 3 : i + 4] for i in (160, 161, 162))
    packed = lat_ref[:, 0:16, :].reshape(512, LN)
    as_float = packed.astype(F32)
    twice = jnp.concatenate([packed, packed], axis=1)
    square = dot(twice, gram_ref[...].reshape(256, LN)) * as_float
    low = low_lanes((512, LN))
    gain_low = lax.rsqrt(jnp.sum(jnp.where(low, square, 0.0), axis=1, keepdims=True) + 1e-06)
    gain_high = lax.rsqrt(jnp.sum(jnp.where(low, 0.0, square), axis=1, keepdims=True) + 1e-06)
    none = jnp.zeros((64, 2 * LN), BF)
    hi, lo = halves(jnp.concatenate([mq, mk], axis=1))
    qk_low = gain_low * dot(twice, jnp.concatenate([hi, none, lo, none], axis=0))
    qk_high = gain_high * dot(twice, jnp.concatenate([none, hi, none, lo], axis=0))
    hi, lo = halves(mv)
    none = jnp.zeros((64, LN), BF)
    for_low = jnp.concatenate([hi, none, lo, none], axis=0)
    for_high = jnp.concatenate([none, hi, none, lo], axis=0)
    v_both = dot(twice, jnp.concatenate([for_low, for_high], axis=1))

    def unit(u, factor):
        mean = jnp.mean(u * u, axis=1, keepdims=True)
        return (u * (lax.rsqrt(mean + 1e-06) * factor)).astype(BF)

    factor = math.log2(math.e) / math.sqrt(128)
    q_low, q_high = (unit(u[:, :LN] + bias_q, factor) for u in (qk_low, qk_high))
    keys = jnp.concatenate([unit(u[:, LN:] + bias_k, 1.0) for u in (qk_low, qk_high)], axis=0)
    values = (
        jnp.concatenate([gain_low * v_both[:, :LN], gain_high * v_both[:, LN:]], axis=0) + bias_v
    )
    all_low = low_lanes((1024, LN))
    values_low = jnp.where(all_low, values, 1.0).astype(BF)
    values_high = jnp.where(all_low, 1.0, values).astype(BF)

    def attend(q, v):
        return dot(jnp.exp2(dot_t(q, keys)).astype(BF), v)

    side = low_lanes((256, LN))
    for core in range(2):
        at = slice(core * 256, core * 256 + 256)
        first = attend(q_low[at], values_low)
        second = attend(q_high[at], values_high)
        over = jnp.where(side, first, second)
        under = pltpu.roll(jnp.where(side, second, first), LN // 2, 1)
        shares = (over / under).astype(BF)
        for z in range(8):
            out_ref[z * 2 + core] = shares[z * 32 : z * 32 + 32]


def step_of(stamps_ref, step):
    width = jnp.full((16, LN), stamps_ref[step + 1] - stamps_ref[step], jnp.int32)
    return width.astype(F32) / 1000.0


def increments_kernel(size_ref, shares_ref, lat_ref, out_ref, own_ref):
    step, side = place(*STEP), place("y_hi")
    velocity = jnp.sum(shares_ref[...].astype(F32), axis=0)
    size = size_ref[...]
    start = jnp.where(step == 0, pack_rows(lat_ref[0]), 0.0)
    for part in range(2):
        mine = velocity[part * 16 : part * 16 + 16]
        grown = size * mine
        grown = jnp.where(side == part, grown + start, grown).astype(BF)
        for peer in range(16):
            out_ref[peer * 2 + part] = grown
    own_ref[...] = jnp.where(side == 0, velocity[:16], velocity[16:])


def finish_kernel(size_ref, terms_ref, own_ref, lat_ref, updated_ref, velocity_ref):
    step, side = place(*STEP), place("y_hi")
    own = own_ref[...]
    size = size_ref[...]
    other = terms_ref[step * 2 + 1 - side].astype(F32)
    start = jnp.where(step == 0, pack_rows(lat_ref[0]), 0.0)
    velocity = own + other / size
    updated = size * own + start + other
    for j in range(15):
        term = terms_ref[2 * j].astype(F32) + terms_ref[2 * j + 1].astype(F32)
        updated = updated + jnp.where(j < step, term, 0.0)
    for ref, value in ((updated_ref, updated), (velocity_ref, velocity)):
        ref[0, 0:16] = value[:, : LN // 2]
        ref[0, 16:32] = pltpu.roll(value, LN // 2, 1)[:, : LN // 2]


def over_x(w, far):
    return lax.ppermute(w, "x", [(i, (i + far) % 4) for i in range(4)])


def near(x):
    return pltpu.with_memory_space_constraint(x, pltpu.VMEM)


def call(kernel, outs, *args, scalars=(), scratch=()):
    smem = pl.BlockSpec(memory_space=pltpu.SMEM)
    vmem = pl.BlockSpec(memory_space=pltpu.VMEM)
    return pl.pallas_call(
        kernel,
        in_specs=[smem] * len(scalars) + [vmem] * len(args),
        out_specs=[vmem] * len(outs),
        out_shape=outs,
        scratch_shapes=scratch,
    )(*scalars, *args)


def stages(latents, timesteps, embed_weight, mod_weight, qkv_weight, out_weight):
    vmem = pltpu.VMEM
    payload, w, size = call(
        pack_kernel,
        [vmem((16, 80, LN), BF), vmem((640, LN), BF), vmem((16, LN), F32)],
        latents,
        mod_weight,
        jnp.moveaxis(qkv_weight[:, 0], 1, 0),
        jnp.swapaxes(out_weight, 1, 2),
        scalars=(timesteps,),
    )
    payload = lax.all_to_all(payload, ("z", "y_hi"), 0, 0, tiled=True)
    gathered = near(lax.all_gather(payload, "core", tiled=True))
    ws = {2: over_x(w, 2)}
    for far in (1, 3):
        ws[far] = over_x(w, far)
    centered, gram = call(
        weights_kernel, [vmem((64, 1024), F32), vmem((2, LN, LN), BF)], near(embed_weight), gathered
    )
    (parts,) = call(
        partial_kernel,
        [vmem((4, 176, LN), BF)],
        gathered,
        near(centered),
        near(w),
        *[near(ws[far]) for far in (1, 2, 3)],
        scratch=[vmem((8, 1024), F32)],
    )
    parts = near(lax.all_to_all(parts, "y_lo", 0, 0, tiled=True))
    (shares,) = call(attend_kernel, [vmem((16, 32, LN), BF)], parts, gathered, near(gram))
    shares = near(lax.all_to_all(shares, ("z", "core"), 0, 0, tiled=True))
    terms, own = call(
        increments_kernel,
        [vmem((32, 16, LN), BF), vmem((16, LN), F32)],
        near(size),
        shares,
        near(latents),
    )
    terms = near(lax.all_to_all(terms, ("y_lo", "x", "y_hi"), 0, 0, tiled=True))
    out = jax.ShapeDtypeStruct(latents.shape, F32)
    return tuple(call(finish_kernel, [out, out], near(size), terms, near(own), near(latents)))


def solution(mesh):
    split = Mesh(mesh.devices.reshape(4, 4, 8, 2, 2), STEP + SEQ)
    return jax.shard_map(
        stages,
        mesh=split,
        in_specs=(
            P(STEP, SEQ, None),
            P(),
            P(),
            P(SEQ, None, None),
            P(STEP, SEQ, None, None),
            P(SEQ, None, None),
        ),
        out_specs=(P(STEP, SEQ, None), P(STEP, SEQ, None)),
        check_vma=False,
    )
```

```python
import math

import jax
import jax.numpy as jnp
from jax import lax
from jax.experimental import pallas as pl
from jax.experimental.pallas import tpu as pltpu
from jax.sharding import Mesh
from jax.sharding import PartitionSpec as P


STEP = ("y_lo", "x")
SEQ = ("z", "y_hi", "core")
BF = jnp.bfloat16
F32 = jnp.float32
LN = 128


def dot(a, b):
    return jnp.dot(a, b, preferred_element_type=F32)


def dot_t(a, b):
    return lax.dot_general(a, b, (((1,), (1,)), ((), ())), preferred_element_type=F32)


def halves(x):
    hi = x.astype(BF)
    return hi, (x - hi.astype(F32)).astype(BF)


def low_lanes(shape):
    return lax.broadcasted_iota(jnp.int32, shape, len(shape) - 1) < LN // 2


def pack_rows(rows):
    return jnp.concatenate([rows[:16], rows[16:]], axis=1)


def place(*axes):
    index = 0
    for axis in axes:
        index = index * lax.axis_size(axis) + lax.axis_index(axis)
    return index


def own_columns():
    return pl.ds(pl.multiple_of(place("y_lo") * 1024, 1024), 1024)


def stamp_at(stamps_ref, index):
    stamps = stamps_ref[...].astype(F32)
    col = lax.broadcasted_iota(jnp.int32, stamps.shape, 1)
    return jnp.sum(jnp.where(col == index, stamps, 0.0), axis=1, keepdims=True)


def step_of(stamps_ref, step):
    return (stamp_at(stamps_ref, step + 1) - stamp_at(stamps_ref, step)) / 1000.0


def conditions(stamps_ref):
    shape = (8, 16)
    row = lax.broadcasted_iota(jnp.int32, shape, 0)
    col = lax.broadcasted_iota(jnp.int32, shape, 1)
    stamp = jnp.zeros(shape, F32)
    for k in range(4):
        stamp = jnp.where(row % 4 == k, stamp_at(stamps_ref, k * 4 + place("x")), stamp)
    feature = place(*SEQ) * 8 + col % 8
    half_count = 128
    frequencies = jnp.exp(-math.log(10000.0) * (feature % half_count).astype(F32) / half_count)
    angles = stamp * frequencies
    value = jnp.where(feature < half_count, jnp.cos(angles), jnp.sin(angles))
    return jnp.where(row // 4 == col // 8, value, 0.0)


def twin(lines):
    low = low_lanes(lines.shape)
    turned = pltpu.roll(lines, LN // 2, 1)
    return jnp.concatenate([jnp.where(low, lines, turned), jnp.where(low, turned, lines)], axis=0)


def pack_kernel(stamps_ref, lat_ref, mw_ref, w_ref, out_weight_ref, out_ref, folded_ref, size_ref):
    size_ref[...] = jnp.broadcast_to(step_of(stamps_ref, place(*STEP)), size_ref.shape)
    out = out_weight_ref[0]
    wv = dot_t(w_ref[2], jnp.concatenate([out, out], axis=0))
    folded_ref[0:512] = w_ref[0:2].reshape(512, LN)
    folded_ref[512:640] = jnp.where(low_lanes((LN, LN)), wv[:LN], wv[LN:]).astype(BF)
    lat = pack_rows(lat_ref[0]).astype(BF)
    own = own_columns()
    cond_hi, cond_lo = halves(conditions(stamps_ref))
    hi, lo = halves(jnp.concatenate([mw_ref[:, 0, own], mw_ref[:, 1, own]], axis=0))
    share = dot(cond_hi, hi) + dot(cond_lo, hi) + dot(cond_hi, lo)
    blocks = [share[:, part * LN : (part + 1) * LN] for part in range(8)]
    payload = jnp.concatenate([lat, jnp.concatenate(blocks, axis=0).astype(BF)], axis=0)
    for peer in range(out_ref.shape[0]):
        out_ref[peer] = payload


def weights_kernel(embed_ref, _, centered_ref, gram_ref):
    embed = embed_ref[...].astype(F32)
    mean = jnp.mean(embed, axis=1, keepdims=True)
    centered_ref[...] = embed_ref[:, own_columns()].astype(F32) - mean
    hi, lo = halves(embed - mean)
    products = dot_t(jnp.concatenate([hi, lo], axis=0), hi)
    cross = products[64:]
    gram = (products[:64] + cross + cross.T) * (1.0 / embed.shape[1])
    none = jnp.zeros_like(gram)
    gram = jnp.concatenate(
        [jnp.concatenate([gram, none], axis=1), jnp.concatenate([none, gram], axis=1)], axis=0
    )
    gram_ref[0], gram_ref[1] = halves(gram)


def partial_kernel(mod_ref, centered_ref, *refs):
    w_refs, out_ref, modulation_ref = refs[:4], refs[4], refs[5]
    total = jnp.sum(mod_ref[:, 16:80, :].astype(F32), axis=0)
    for part in range(8):
        modulation_ref[:, part * LN : (part + 1) * LN] = total[part * 8 : part * 8 + 8]
    m_qk = m_v = 0.0
    for far, w_ref in enumerate(w_refs):
        origin = lax.rem(place("x") + 4 - far, 4)
        own = pl.ds(pl.multiple_of(origin * 256, 256), 256)
        modulation = modulation_ref[:, own]
        shift, scale = modulation[:4], modulation[4:]
        centered = centered_ref[:, own]
        scaled = [(centered * scale[k : k + 1]).astype(BF) for k in range(4)]
        shifts = jnp.concatenate([*halves(shift), jnp.zeros((8, 256), BF)], axis=0)
        rows = jnp.concatenate([*halves(centered), *scaled, shifts], axis=0)
        m_qk = m_qk + dot(rows, jnp.concatenate([w_ref[0:256], w_ref[256:512]], axis=1))
        m_v = m_v + dot(rows, twin(w_ref[512:640].astype(F32)).astype(BF))
    line = lax.broadcasted_iota(jnp.int32, (16, LN), 0)
    low = low_lanes((32, LN))
    plain_qk = m_qk[0:64] + m_qk[64:128]
    plain_v = m_v[0:64] + m_v[64:128]
    for k in range(4):
        at = slice(128 + k * 64, 192 + k * 64)
        qk = plain_qk + m_qk[at]
        v = plain_v + m_v[at]
        out_ref[k, 0:64] = qk[:, :LN].astype(BF)
        out_ref[k, 64:128] = qk[:, LN:].astype(BF)
        out_ref[k, 128:160] = jnp.where(low, v[:32], v[32:]).astype(BF)
        hi, lo = slice(384 + k, 385 + k), slice(388 + k, 389 + k)
        b_qk, b_v = m_qk[hi] + m_qk[lo], m_v[hi] + m_v[lo]
        tile = jnp.zeros((16, LN), F32)
        for i, bias in enumerate((b_qk[:, :LN], b_qk[:, LN:], b_v)):
            rounded = bias.astype(BF).astype(F32)
            tile = jnp.where(line == i, rounded, tile)
            tile = jnp.where(line == i + 3, bias - rounded, tile)
        out_ref[k, 160:176] = tile.astype(BF)


def attend_kernel(parts_ref, lat_ref, gram_ref, out_ref):
    total = jnp.sum(parts_ref[...].astype(F32), axis=0)
    mq, mk, mv = total[0:64], total[64:128], total[128:160]
    mv = twin(mv)
    bias_q, bias_k, bias_v = (total[i : i + 1] + total[i + 3 : i + 4] for i in (160, 161, 162))
    packed = lat_ref[:, 0:16, :].reshape(512, LN)
    as_float = packed.astype(F32)
    twice = jnp.concatenate([packed, packed], axis=1)
    square = dot(twice, gram_ref[...].reshape(256, LN)) * as_float
    low = low_lanes((512, LN))
    gain_low = lax.rsqrt(jnp.sum(jnp.where(low, square, 0.0), axis=1, keepdims=True) + 1e-06)
    gain_high = lax.rsqrt(jnp.sum(jnp.where(low, 0.0, square), axis=1, keepdims=True) + 1e-06)
    none = jnp.zeros((64, 2 * LN), BF)
    hi, lo = halves(jnp.concatenate([mq, mk], axis=1))
    qk_low = gain_low * dot(twice, jnp.concatenate([hi, none, lo, none], axis=0))
    qk_high = gain_high * dot(twice, jnp.concatenate([none, hi, none, lo], axis=0))
    hi, lo = halves(mv)
    none = jnp.zeros((64, LN), BF)
    for_low = jnp.concatenate([hi, none, lo, none], axis=0)
    for_high = jnp.concatenate([none, hi, none, lo], axis=0)
    v_both = dot(twice, jnp.concatenate([for_low, for_high], axis=1))

    def unit(u, factor):
        mean = jnp.mean(u * u, axis=1, keepdims=True)
        return (u * (lax.rsqrt(mean + 1e-06) * factor)).astype(BF)

    factor = math.log2(math.e) / math.sqrt(128)
    q_low, q_high = (unit(u[:, :LN] + bias_q, factor) for u in (qk_low, qk_high))
    keys = jnp.concatenate([unit(u[:, LN:] + bias_k, 1.0) for u in (qk_low, qk_high)], axis=0)
    values = (
        jnp.concatenate([gain_low * v_both[:, :LN], gain_high * v_both[:, LN:]], axis=0) + bias_v
    )
    all_low = low_lanes((1024, LN))
    values_low = jnp.where(all_low, values, 1.0).astype(BF)
    values_high = jnp.where(all_low, 1.0, values).astype(BF)

    def attend(q, v):
        return dot(jnp.exp2(dot_t(q, keys)).astype(BF), v)

    side = low_lanes((256, LN))
    for core in range(2):
        at = slice(core * 256, core * 256 + 256)
        first = attend(q_low[at], values_low)
        second = attend(q_high[at], values_high)
        over = jnp.where(side, first, second)
        under = pltpu.roll(jnp.where(side, second, first), LN // 2, 1)
        shares = (over / under).astype(BF)
        for z in range(8):
            out_ref[z * 2 + core] = shares[z * 32 : z * 32 + 32]


def increments_kernel(size_ref, shares_ref, lat_ref, out_ref, own_ref):
    step, side = place(*STEP), place("y_hi")
    velocity = jnp.sum(shares_ref[...].astype(F32), axis=0)
    size = size_ref[...]
    start = jnp.where(step == 0, pack_rows(lat_ref[0]), 0.0)
    for part in range(2):
        mine = velocity[part * 16 : part * 16 + 16]
        grown = size * mine
        grown = jnp.where(side == part, grown + start, grown).astype(BF)
        for peer in range(16):
            out_ref[peer * 2 + part] = grown
    own_ref[...] = jnp.where(side == 0, velocity[:16], velocity[16:])


def finish_kernel(size_ref, terms_ref, own_ref, lat_ref, updated_ref, velocity_ref):
    step, side = place(*STEP), place("y_hi")
    own = own_ref[...]
    size = size_ref[...]
    other = terms_ref[step * 2 + 1 - side].astype(F32)
    start = jnp.where(step == 0, pack_rows(lat_ref[0]), 0.0)
    velocity = own + other / size
    updated = size * own + start + other
    for j in range(15):
        term = terms_ref[2 * j].astype(F32) + terms_ref[2 * j + 1].astype(F32)
        updated = updated + jnp.where(j < step, term, 0.0)
    for ref, value in ((updated_ref, updated), (velocity_ref, velocity)):
        ref[0, 0:16] = value[:, : LN // 2]
        ref[0, 16:32] = pltpu.roll(value, LN // 2, 1)[:, : LN // 2]


def over_x(w, far):
    return lax.ppermute(w, "x", [(i, (i + far) % 4) for i in range(4)])


def near(x):
    return pltpu.with_memory_space_constraint(x, pltpu.VMEM)


def call(kernel, outs, *args, scalars=(), scratch=()):
    smem = pl.BlockSpec(memory_space=pltpu.SMEM)
    vmem = pl.BlockSpec(memory_space=pltpu.VMEM)
    return pl.pallas_call(
        kernel,
        in_specs=[smem] * len(scalars) + [vmem] * len(args),
        out_specs=[vmem] * len(outs),
        out_shape=outs,
        scratch_shapes=scratch,
    )(*scalars, *args)


def stages(latents, timesteps, embed_weight, mod_weight, qkv_weight, out_weight):
    vmem = pltpu.VMEM
    payload, w, size = call(
        pack_kernel,
        [vmem((16, 80, LN), BF), vmem((640, LN), BF), vmem((16, LN), F32)],
        timesteps[None],
        latents,
        mod_weight,
        jnp.moveaxis(qkv_weight[:, 0], 1, 0),
        jnp.swapaxes(out_weight, 1, 2),
    )
    payload = lax.all_to_all(payload, ("z", "y_hi"), 0, 0, tiled=True)
    gathered = near(lax.all_gather(payload, "core", tiled=True))
    ws = {2: over_x(w, 2)}
    for far in (1, 3):
        ws[far] = over_x(w, far)
    centered, gram = call(
        weights_kernel, [vmem((64, 1024), F32), vmem((2, LN, LN), BF)], near(embed_weight), gathered
    )
    (parts,) = call(
        partial_kernel,
        [vmem((4, 176, LN), BF)],
        gathered,
        near(centered),
        near(w),
        *[near(ws[far]) for far in (1, 2, 3)],
        scratch=[vmem((8, 1024), F32)],
    )
    parts = near(lax.all_to_all(parts, "y_lo", 0, 0, tiled=True))
    (shares,) = call(attend_kernel, [vmem((16, 32, LN), BF)], parts, gathered, near(gram))
    shares = near(lax.all_to_all(shares, ("z", "core"), 0, 0, tiled=True))
    terms, own = call(
        increments_kernel,
        [vmem((32, 16, LN), BF), vmem((16, LN), F32)],
        near(size),
        shares,
        near(latents),
    )
    terms = near(lax.all_to_all(terms, ("y_lo", "x", "y_hi"), 0, 0, tiled=True))
    out = jax.ShapeDtypeStruct(latents.shape, F32)
    return tuple(call(finish_kernel, [out, out], near(size), terms, near(own), near(latents)))


def solution(mesh):
    split = Mesh(mesh.devices.reshape(4, 4, 8, 2, 2), STEP + SEQ)
    return jax.shard_map(
        stages,
        mesh=split,
        in_specs=(
            P(STEP, SEQ, None),
            P(),
            P(),
            P(SEQ, None, None),
            P(STEP, SEQ, None, None),
            P(SEQ, None, None),
        ),
        out_specs=(P(STEP, SEQ, None), P(STEP, SEQ, None)),
        check_vma=False,
    )
```
